32 devices in a mesh: mesh: 4 (over z), rve: 8 (over y, x, core).
Axes of the slice: x: 2, y: 2, z: 4, core: 2. Of those that a mesh axis runs over, the one named last changes fastest.
Arguments:
- displacement: float32 [3, 128], P(None, ('mesh', 'rve')), may hold values from -6 to 6
- shape_grads: float32 [3, 8, 512], P(None, None, ('mesh', 'rve')), may hold values from -2 to 2
- point_weights: float32 [512], P(('mesh', 'rve')), may hold values from 0.5 to 2
- conn: int32 [8, 64], P(None, ('mesh', 'rve')), may hold values from 0 to 47
- halo_nodes: int32 [2, 32], P(None, 'mesh'), may hold values from 0 to 31
- warm_strain: float32 [512, 6, 4096], P(('mesh', 'rve')), may hold values from -4 to 4
- moduli: float32 [512, 2, 4096], P(('mesh', 'rve')), may hold values from 0.2 to 2
- owner: int32 [512], P(('mesh', 'rve')), may hold values from 0 to 7, as said below
- sweeps: int32 [512], P(('mesh', 'rve')), may hold values from 1 to 2, as said below
Outputs:
- nodal_force: float32 [3, 128], P(None, ('mesh', 'rve'))
- gp_stress: float32 [6, 512], P(None, ('mesh', 'rve'))
- micro_strain: float32 [512, 6, 4096], P(('mesh', 'rve'))
The draws below stay inside these ranges and needn't reach their ends.
Inputs may be any that keep to these rules, and one draw needn't show every extreme that they name: The owner lies in the Gauss point's own mesh row. The 16 Gauss points of one device go 2 each to 8 different owners, and every owner receives exactly 16 Gauss points. `sweeps`: counts may be skewed by owner: all Gauss points of some owners take 2.
All inputs are finite; a program needn't handle non-finite values.
Results may differ from the reference program's by a relative error of at most 0.0003.
Values sent between devices are 32-bit elements; how exact they have to be, the bound alone decides.
No kernel may reach another device: no remote copies, remote signals or barrier semaphores. Data moves between devices by JAX's collectives and lax.ppermute only.
A program may use at most 128 MiB of HBM per device.

```python
import math
import jax
import jax.numpy as jnp
from jax import lax

RES = 16
VOX = 4096
GP_DEV = 16
CAP = 2
NODE_DEV = 4
HALO = 8
GPS = 512
ELEMS = 64
NODES = 128
N_MESH = 4
N_RVE = 8


def shared_routes(key):
    base = jax.random.fold_in(key, 11)
    row_count = GPS // (N_RVE * GP_DEV)
    key_list = jax.random.split(base, 4)
    shift_order = jax.vmap(lambda subkey: jax.random.permutation(subkey, N_RVE))(jax.random.split(key_list[0], row_count))
    slot_order = jax.vmap(lambda subkey: jax.random.permutation(subkey, GP_DEV))(jax.random.split(key_list[1], row_count * N_RVE))
    slot_order = slot_order.reshape(row_count, N_RVE, GP_DEV)
    group_index = slot_order // CAP
    owners = (shift_order[:, :, None] + group_index) % N_RVE
    heavy_rank = jax.vmap(lambda subkey: jax.random.permutation(subkey, N_RVE))(jax.random.split(key_list[2], row_count))
    owner_rank = jnp.take_along_axis(heavy_rank, owners.reshape(row_count, N_RVE * GP_DEV), axis=1)
    heavy_owner = owner_rank.reshape(row_count, N_RVE, GP_DEV) < max(1, N_RVE // 8)
    light_count = 1 + (jax.random.randint(key_list[3], (row_count, N_RVE, GP_DEV), 0, 4) == 0).astype(jnp.int32)
    counts = jnp.where(heavy_owner, 2, light_count)
    return (owners.reshape(GPS).astype(jnp.int32), counts.reshape(GPS).astype(jnp.int32))


def draw_owner(key, part):
    return shared_routes(key)[0]


def draw_sweeps(key, part):
    return shared_routes(key)[1]


def plant(values, stream_key, low, top_value):
    longest = values.shape.index(max(values.shape))
    spots = []
    for shift in (0, 1):
        where = [jax.random.randint(jax.random.fold_in(stream_key, axis), (), 0, length) for axis, length in enumerate(values.shape)]
        where[longest] = (where[longest] + shift) % values.shape[longest]
        spots.append(tuple(where))
    return values.at[spots[0]].set(low).at[spots[1]].set(top_value)


def block_scale(stream_key, dims, shards, smallest, high):
    loudness, own = 1.0, jax.random.fold_in(stream_key, 6)
    for axis_at, shards_of in shards:
        draws = jnp.exp(jax.random.uniform(jax.random.fold_in(own, axis_at), (shards_of,), jnp.float32, smallest / len(shards), high / len(shards)))
        loudness = loudness * jnp.repeat(draws, dims[axis_at] // shards_of).reshape([-1 if axis == axis_at else 1 for axis in range(len(dims))])
    return loudness


def noise(rng, extent, scale, bound, pieces=(), held_as=jnp.bfloat16):
    drawn = scale * jax.random.normal(rng, extent, jnp.float32)
    if pieces:
        drawn = drawn * block_scale(rng, extent, pieces, -0.22, 0.18)
    return jnp.clip(drawn, -bound, bound).astype(held_as)


def setup_inputs(seed: int = 0) -> dict:
    seeds = jax.random.split(jax.random.key(seed), 10)
    displacement = noise(seeds[0], (3, NODES), 1.0, 6.0, ((1, 32),), jnp.float32)
    shape_grads = noise(seeds[1], (3, 8, GPS), 8 ** -0.5, 2.0, ((2, 32),), jnp.float32)
    point_weights = jnp.clip(jnp.exp(math.log(2.0) - 1.3862944 * jax.random.uniform(seeds[2], (GPS,), jnp.float32) ** block_scale(seeds[2], (GPS,), ((0, 32),), -0.2, 0.2)), 0.5, 2.0)
    conn = plant(jax.random.randint(seeds[3], (8, ELEMS), 0, NODE_DEV * N_RVE + 2 * HALO), jax.random.fold_in(seeds[3], 1), 0, (NODE_DEV * N_RVE + 2 * HALO) - 1).astype(jnp.int32)
    halo_nodes = plant(jax.random.randint(seeds[4], (2, HALO * N_MESH), 0, NODE_DEV * N_RVE), jax.random.fold_in(seeds[4], 1), 0, (NODE_DEV * N_RVE) - 1).astype(jnp.int32)
    warm_strain = noise(seeds[5], (GPS, 6, VOX), 0.5, 4.0, ((0, 32),), jnp.float32)
    moduli = jnp.clip(jnp.exp(math.log(2.0) - 2.3025851 * jax.random.uniform(seeds[6], (GPS, 2, VOX), jnp.float32) ** block_scale(seeds[6], (GPS, 2, VOX), ((0, 32),), -0.2, 0.2)), 0.2, 2.0)
    owner = draw_owner(jax.random.fold_in(seeds[9], 71), 0)
    sweeps = draw_sweeps(jax.random.fold_in(seeds[9], 71), 0)
    return {"displacement": displacement, "shape_grads": shape_grads, "point_weights": point_weights, "conn": conn, "halo_nodes": halo_nodes, "warm_strain": warm_strain, "moduli": moduli, "owner": owner, "sweeps": sweeps}


ref_modulus = 1.1
half_inverse = 1.0 / 2.2
coupling = 2.2 / (1.1 * 3.3)
index_pairs = ((0, 0), (1, 1), (2, 2), (1, 2), (0, 2), (0, 1))
diagonal_entries = (1.0, 1.0, 1.0, 0.0, 0.0, 0.0)

def unit_normals(grid_side):
    wave = jnp.arange(grid_side, dtype=jnp.int32)
    signed = jnp.where(wave < grid_side // 2, wave, wave - grid_side).astype(jnp.float32)
    cube = (grid_side, grid_side, grid_side)
    along_x = jnp.broadcast_to(signed[:, None, None], cube).reshape(-1)
    along_y = jnp.broadcast_to(signed[None, :, None], cube).reshape(-1)
    along_z = jnp.broadcast_to(signed[None, None, :], cube).reshape(-1)
    length_sq = along_x * along_x + along_y * along_y + along_z * along_z
    safe_length = jnp.sqrt(jnp.where(length_sq > 0, length_sq, 1.0))
    inverse_len = jnp.where(length_sq > 0, 1.0 / safe_length, 0.0)
    return jnp.stack([along_x * inverse_len, along_y * inverse_len, along_z * inverse_len])

def green_apply(polar, normals):
    vectors = (normals[0], normals[1], normals[2])
    entries = [polar[..., component, :] for component in range(6)]
    traction_x = entries[0] * vectors[0] + entries[5] * vectors[1] + entries[4] * vectors[2]
    traction_y = entries[5] * vectors[0] + entries[1] * vectors[1] + entries[3] * vectors[2]
    traction_z = entries[4] * vectors[0] + entries[3] * vectors[1] + entries[2] * vectors[2]
    tractions = (traction_x, traction_y, traction_z)
    normal_load = vectors[0] * traction_x + vectors[1] * traction_y + vectors[2] * traction_z
    result = []
    for first_axis, second_axis in index_pairs:
        pair_term = vectors[first_axis] * tractions[second_axis] + vectors[second_axis] * tractions[first_axis]
        result.append(pair_term * half_inverse - coupling * vectors[first_axis] * vectors[second_axis] * normal_load)
    return jnp.stack(result, axis=-2)

def stress_of(strain_field, lame_first, shear_modulus):
    trace_sum = strain_field[:, 0] + strain_field[:, 1] + strain_field[:, 2]
    diagonal_mask = jnp.array(diagonal_entries, jnp.float32)
    return 2.0 * shear_modulus[:, None, :] * strain_field + (lame_first * trace_sum)[:, None, :] * diagonal_mask[None, :, None]

def sweep_once(strain_field, macro_rows, lame_first, shear_modulus, normals):
    batch_size = strain_field.shape[0]
    trace_sum = strain_field[:, 0] + strain_field[:, 1] + strain_field[:, 2]
    diagonal_mask = jnp.array(diagonal_entries, jnp.float32)
    polar = 2.0 * (shear_modulus - ref_modulus)[:, None, :] * strain_field
    polar = polar + ((lame_first - ref_modulus) * trace_sum)[:, None, :] * diagonal_mask[None, :, None]
    spectrum = jnp.fft.fftn(polar.reshape(batch_size, 6, RES, RES, RES), axes=(2, 3, 4)).reshape(batch_size, 6, VOX)
    real_green = green_apply(spectrum.real, normals)
    imag_green = green_apply(spectrum.imag, normals)
    merged = lax.complex(real_green, imag_green).reshape(batch_size, 6, RES, RES, RES)
    fluctuation = jnp.fft.ifftn(merged, axes=(2, 3, 4)).real.reshape(batch_size, 6, VOX)
    return macro_rows[:, :, None] - fluctuation

def reference(displacement, shape_grads, point_weights, conn, halo_nodes, warm_strain, moduli, owner, sweeps):
    row_count = N_MESH
    part_nodes = NODE_DEV * N_RVE
    per_part = ELEMS // row_count
    highest = lax.Precision.HIGHEST
    moved = displacement.reshape(3, row_count, part_nodes).transpose(1, 0, 2)
    lists = halo_nodes.reshape(2, row_count, HALO)
    down_values = jax.vmap(lambda table, picks: table[:, picks])(moved, lists[0])
    up_values = jax.vmap(lambda table, picks: table[:, picks])(moved, lists[1])
    zero_face = jnp.zeros((1, 3, HALO), jnp.float32)
    from_below = jnp.concatenate([zero_face, up_values[:-1]], axis=0)
    from_above = jnp.concatenate([down_values[1:], zero_face], axis=0)
    extended = jnp.concatenate([moved, from_below, from_above], axis=2)
    links = conn.reshape(8, row_count, per_part).transpose(1, 0, 2)
    elem_disp = jax.vmap(lambda table, picks: table[:, picks])(extended, links)
    gradients = shape_grads.reshape(3, 8, row_count, per_part, 8)
    grad_disp = jnp.einsum('piae,japeq->ijpeq', elem_disp, gradients, precision=highest).reshape(3, 3, GPS)
    macro_strain = jnp.stack([grad_disp[0, 0], grad_disp[1, 1], grad_disp[2, 2], (grad_disp[1, 2] + grad_disp[2, 1]) * 0.5, (grad_disp[0, 2] + grad_disp[2, 0]) * 0.5, (grad_disp[0, 1] + grad_disp[1, 0]) * 0.5])
    normals = unit_normals(RES)

    def solve_block(operands):
        macro_rows, warm_rows, moduli_rows, count_rows = operands
        lame_first = moduli_rows[:, 0]
        shear_modulus = moduli_rows[:, 1]
        strain_field = warm_rows - lax.optimization_barrier(jnp.mean(warm_rows, axis=2, keepdims=True)) + macro_rows[:, :, None]
        for sweep_index in range(2):
            updated = sweep_once(strain_field, macro_rows, lame_first, shear_modulus, normals)
            strain_field = jnp.where((count_rows > sweep_index)[:, None, None], updated, strain_field)
        mean_stress = lax.optimization_barrier(jnp.mean(stress_of(strain_field, lame_first, shear_modulus), axis=2))
        return (strain_field, mean_stress)
    blocks = GPS // GP_DEV
    operands = (macro_strain.T.reshape(blocks, GP_DEV, 6), warm_strain.reshape(blocks, GP_DEV, 6, VOX), moduli.reshape(blocks, GP_DEV, 2, VOX), sweeps.reshape(blocks, GP_DEV))
    strain_all, stress_all = lax.map(solve_block, operands)
    strain_all = strain_all.reshape(GPS, 6, VOX)
    gp_stress = stress_all.reshape(GPS, 6).T
    point_index = jnp.arange(GPS, dtype=jnp.int32)
    row_of = point_index // (GP_DEV * N_RVE)
    sort_keys = (row_of * N_RVE + owner.astype(jnp.int32)) * GPS + point_index
    order = jnp.argsort(sort_keys, stable=True).astype(jnp.int32)
    micro_strain = strain_all[order]
    comps = gp_stress
    symmetric = jnp.stack([jnp.stack([comps[0], comps[5], comps[4]]), jnp.stack([comps[5], comps[1], comps[3]]), jnp.stack([comps[4], comps[3], comps[2]])])
    weighted = symmetric * point_weights[None, None, :]
    element_force = jnp.einsum('ijpeq,japeq->piae', weighted.reshape(3, 3, row_count, per_part, 8), gradients, precision=highest)
    width_ext = part_nodes + 2 * HALO
    spread = jax.vmap(lambda forces, picks: jnp.zeros((3, width_ext), jnp.float32).at[:, picks].add(forces))(element_force, links)
    own_part = spread[:, :, :part_nodes]
    below_part = spread[:, :, part_nodes:part_nodes + HALO]
    above_part = spread[:, :, part_nodes + HALO:]
    incoming_low = jnp.concatenate([zero_face, above_part[:-1]], axis=0)
    incoming_high = jnp.concatenate([below_part[1:], zero_face], axis=0)

    def settle(own_rows, low_rows, high_rows, low_list, high_list):
        return own_rows.at[:, low_list].add(low_rows).at[:, high_list].add(high_rows)
    own_part = jax.vmap(settle)(own_part, incoming_low, incoming_high, lists[0], lists[1])
    nodal_force = own_part.transpose(1, 0, 2).reshape(3, NODES)
    return (nodal_force, gp_stress, micro_strain)
```

```python
import functools
import math

import jax
import jax.numpy as jnp
import numpy as np
from jax import lax
from jax.experimental import pallas as pl
from jax.experimental.pallas import tpu as pltpu
from jax.sharding import PartitionSpec as P

REF_MODULUS = 1.1
COUPLING = 2.2 / (1.1 * 3.3)
PAIRS = ((0, 0), (1, 1), (2, 2), (1, 2), (0, 2), (0, 1))
F32 = jnp.float32
BF16 = jnp.bfloat16
LANES = 128


def signed_waves(side):
    wave = np.arange(side)
    return np.where(wave < side // 2, wave, wave - side)


def normal_at(kx, ky, kz, side):
    signed = signed_waves(side)
    xi = np.stack([signed[kx % side], signed[ky % side], signed[kz % side]]).astype(np.float64)
    length = np.sqrt((xi * xi).sum(0))
    return np.where(length > 0, xi / np.where(length > 0, length, 1.0), 0.0)


def plane_sets(side):
    packs = []
    for parity in (0, 1):
        reps, selfs, seen = [], [], set()
        for ky in range(parity, side, 2):
            for kz in range(side):
                if (ky, kz) in seen:
                    continue
                mirror = (-ky % side, -kz % side)
                seen.update({(ky, kz), mirror})
                (selfs if mirror == (ky, kz) else reps).append((ky, kz))
        half = len(selfs) // 2
        first = reps + selfs[:half]
        second = reps + selfs[half:]
        packs.append((first, second, len(reps)))
    return packs


def split_table(table):
    high = np.asarray(table, np.float32).astype(jnp.bfloat16)
    low = (np.asarray(table, np.float64) - high.astype(np.float64)).astype(jnp.bfloat16)
    return high, low


def build_tables(side):
    plane = side * side
    half = plane // 2
    ylo, zz = np.divmod(np.arange(half), side)
    scale = 1.0 / (2.2 * side**3)
    forward = np.zeros((2, 2, plane, plane))
    inverse = np.zeros((2, 2, plane, plane))
    normals = np.zeros((2, side // 2, 2, 6, half))
    packs = plane_sets(side)
    for parity in (0, 1):
        kyi, kz = np.divmod(np.arange(half), side)
        ky = 2 * kyi + parity
        angle = 2 * np.pi / side * ((np.outer(ylo, ky) + np.outer(zz, kz)) % side)
        c, s = np.cos(angle), np.sin(angle)
        forward[parity, 1] = np.block([[c, -s], [s, c]])
        inverse[parity, 1] = np.block([[c.T, s.T], [-s.T, c.T]]) * scale
        for kx in range(1, side // 2):
            plus = normal_at(np.full(half, kx), ky, kz, side)
            minus = normal_at(np.full(half, -kx), -ky, -kz, side)
            normals[parity, kx, :, 0:3] = plus
            normals[parity, kx, :, 3:6] = minus
        first, second, pairs = packs[parity]
        columns = np.array(first + second)
        angle = 2 * np.pi / side * (
            (np.outer(ylo, columns[:, 0]) + np.outer(zz, columns[:, 1])) % side
        )
        imag = np.zeros(half, bool)
        imag[half // 2 : half // 2 + pairs] = True
        single = np.zeros(half, bool)
        single[pairs : half // 2] = True
        single[half // 2 + pairs :] = True
        fwd = np.where(imag[None], -np.sin(angle), np.cos(angle))
        inv = (fwd * np.where(single, 1.0, 2.0)[None]).T * scale
        forward[parity, 0, :half, :half] = fwd
        forward[parity, 0, half:, half:] = fwd
        inverse[parity, 0, :half, :half] = inv
        inverse[parity, 0, half:, half:] = inv
        for part, kx in ((0, 0), (1, side // 2)):
            full = np.full(half, kx)
            normals[parity, 0, part, 0:3] = normal_at(full, columns[:, 0], columns[:, 1], side)
            normals[parity, 0, part, 3:6] = normal_at(-full, -columns[:, 0], -columns[:, 1], side)
    fh, fl = split_table(forward)
    ih, il = split_table(inverse)
    return fh, fl, ih, il, normals.astype(np.float32)


def real_transform(values):
    count = len(values)
    if count == 2:
        return [(values[0] + values[1], None), (values[0] - values[1], None)]
    even = real_transform(values[0::2])
    odd = real_transform(values[1::2])
    half = count // 2
    result = [None] * (half + 1)
    result[0] = (even[0][0] + odd[0][0], None)
    result[half] = (even[0][0] - odd[0][0], None)
    for k in range(1, half // 2):
        (er, ei), (orr, oi) = even[k], odd[k]
        angle = 2 * math.pi * k / count
        c, s = math.cos(angle), math.sin(angle)
        if abs(c - s) < 1e-9:
            tr, ti = (orr + oi) * c, (oi - orr) * c
        else:
            tr, ti = orr * c + oi * s, oi * c - orr * s
        result[k] = (er + tr, ei + ti)
        result[half - k] = (er - tr, ti - ei)
    result[half // 2] = (even[half // 2][0], -odd[half // 2][0])
    return result


def real_inverse(spectrum):
    half = len(spectrum) - 1
    count = 2 * half
    if count == 2:
        return [spectrum[0][0] + spectrum[1][0], spectrum[0][0] - spectrum[1][0]]
    even = [None] * (half // 2 + 1)
    odd = [None] * (half // 2 + 1)
    even[0] = (spectrum[0][0] + spectrum[half][0], None)
    odd[0] = (spectrum[0][0] - spectrum[half][0], None)
    for k in range(1, half // 2):
        (ar, ai), (br, bi) = spectrum[k], spectrum[half - k]
        even[k] = (ar + br, ai - bi)
        dr, di = ar - br, ai + bi
        angle = 2 * math.pi * k / count
        c, s = math.cos(angle), math.sin(angle)
        if abs(c - s) < 1e-9:
            odd[k] = ((dr - di) * c, (dr + di) * c)
        else:
            odd[k] = (dr * c - di * s, dr * s + di * c)
    mid_re, mid_im = spectrum[half // 2]
    even[half // 2] = (mid_re * 2.0, None)
    odd[half // 2] = (mid_im * -2.0, None)
    first, second = real_inverse(even), real_inverse(odd)
    result = []
    for a, b in zip(first, second):
        result += [a, b]
    return result


def green(entries, normal):
    n0, n1, n2 = normal
    t0 = entries[0] * n0 + entries[5] * n1 + entries[4] * n2
    t1 = entries[5] * n0 + entries[1] * n1 + entries[3] * n2
    t2 = entries[4] * n0 + entries[3] * n1 + entries[2] * n2
    load = (n0 * t0 + n1 * t1 + n2 * t2) * (COUPLING * 1.1)
    u0, u1, u2 = t0 - n0 * load, t1 - n1 * load, t2 - n2 * load
    return (
        n0 * u0, n1 * u1, n2 * u2,
        n1 * u2 + n2 * u1, n0 * u2 + n2 * u0, n0 * u1 + n1 * u0,
    )


def split_rows(value):
    high = value.astype(BF16)
    return high, (value - high.astype(F32)).astype(BF16)


def product(high, low, table_high, table_low):
    dot = functools.partial(jnp.dot, preferred_element_type=F32)
    return dot(high, table_high) + (dot(low, table_high) + dot(high, table_low))


def column_to_row(column, diagonal):
    return jnp.sum(jnp.where(diagonal, column, 0.0), axis=0, keepdims=True)


def row_to_column(row, diagonal):
    return jnp.sum(jnp.where(diagonal, row, 0.0), axis=1, keepdims=True)


def main_kernel(
    dims,
    part_ref, ids_ref, conn_ref, grads_ref, table_ref, warm_ref, lame_ref, shear_ref,
    fh_ref, fl_ref, ih_ref, il_ref, normals_ref,
    send_ref, stress_ref, force_ref,
    field, tau, lamb, shear, high, low, spec,
):
    points, comps, side, devices, node_dev, halo, row_span, nodes_part, owners, dense = dims
    voxels = side**3
    plane = side * side
    tiles = voxels // LANES
    rows = comps * points
    slabs = side // 2
    part = part_ref[0]

    lane = lax.broadcasted_iota(jnp.int32, (points, LANES), 1)
    sub = lax.broadcasted_iota(jnp.int32, (points, LANES), 0)
    diagonal = lane == sub
    owner_row = ids_ref[0:1, :]
    sweeps_row = ids_ref[1:2, :]
    weight_row = ids_ref[2:3, :]
    valid = lane < points
    if dense:
        owner_col = row_to_column(owner_row, diagonal)
        earlier = jnp.where((owner_col == owner_row) & (lane < sub), 1.0, 0.0)
        rank_col = jnp.sum(earlier, axis=1, keepdims=True)
        slot_row = column_to_row(rank_col * owners + owner_col, diagonal)
        choose = jnp.where((slot_row == sub.astype(F32)) & valid, 1.0, 0.0)
    else:
        choose = jnp.where(diagonal, 1.0, 0.0)
    pick_col = jnp.sum(choose * lane.astype(F32), axis=1, keepdims=True).astype(jnp.int32)
    count_col = jnp.sum(choose * sweeps_row, axis=1, keepdims=True)

    exch = table_ref[...]
    dev_sub = lax.broadcasted_iota(jnp.int32, exch.shape, 0)
    below = jnp.sum(jnp.where(dev_sub == (part - 1) * row_span, exch, 0.0), axis=0, keepdims=True)
    above = jnp.sum(jnp.where(dev_sub == (part + 1) * row_span, exch, 0.0), axis=0, keepdims=True)
    parts = devices // row_span
    width = nodes_part + 2 * halo
    wide = table_ref.shape[1]
    elane = lax.broadcasted_iota(jnp.int32, (1, wide), 1)
    lane_f = elane.astype(F32)
    part_f = part.astype(F32)
    span = float(nodes_part)
    low_id = jnp.where(part > 0, below + (part_f - 1.0) * span, -1.0)
    high_id = jnp.where(part < parts - 1, above + (part_f + 1.0) * span, -1.0)
    node_row = jnp.where(
        elane < nodes_part,
        part_f * span + lane_f,
        jnp.where(elane < nodes_part + halo, low_id, high_id),
    )
    links = conn_ref[...]
    node_col = jnp.sum(jnp.where(links == elane, node_row, 0.0), axis=1, keepdims=True)
    device_col = jnp.floor(node_col * (1.0 / node_dev))
    inner_col = node_col - device_col * node_dev
    nlinks = links.shape[0]
    hit_lane = lax.broadcasted_iota(jnp.int32, (nlinks, devices), 1).astype(F32)
    hit = jnp.where(hit_lane == device_col, 1.0, 0.0)
    flat_lane = lax.broadcasted_iota(jnp.int32, (nlinks, LANES), 1)
    group = flat_lane // node_dev
    inside = jnp.where(
        ((flat_lane - group * node_dev).astype(F32) == inner_col) & (group < 3), 1.0, 0.0
    )
    fetched = jnp.dot(hit, exch[:, :LANES], preferred_element_type=F32,
                      precision=lax.Precision.HIGHEST) * inside
    moved = [
        jnp.sum(jnp.where(group == i, fetched, 0.0), axis=1, keepdims=True) for i in range(3)
    ]
    elements = points // 8
    glane = lax.broadcasted_iota(jnp.int32, (8, LANES), 1)
    spread = []
    for i in range(3):
        acc = jnp.zeros((8, LANES), F32)
        for e in range(elements):
            acc = jnp.where(glane // 8 == e, moved[i][8 * e : 8 * e + 8], acc)
        spread.append(acc)
    grads = [grads_ref[j] for j in range(3)]
    grad = [
        [jnp.sum(spread[i] * grads[j], axis=0, keepdims=True) for j in range(3)] for i in range(3)
    ]
    macro_rows = [grad[0][0], grad[1][1], grad[2][2]] + [
        (grad[a][b] + grad[b][a]) * 0.5 for a, b in PAIRS[3:]
    ]
    macro_cols = [jnp.sum(choose * row, axis=1, keepdims=True) for row in macro_rows]

    octets = points // 8
    picks = [
        jnp.broadcast_to(pick_col[8 * o : 8 * o + 8], (8, LANES)) for o in range(octets)
    ]

    def gather(ref_value):
        if not dense:
            return ref_value
        outs = []
        for o in range(octets):
            best = None
            for source in range(octets):
                local = jnp.clip(picks[o] - 8 * source, 0, 7)
                got = jnp.take_along_axis(
                    ref_value[8 * source : 8 * source + 8], local, axis=0,
                    mode="promise_in_bounds",
                )
                best = got if best is None else jnp.where(picks[o] >= 8 * source, got, best)
            outs.append(best)
        return jnp.concatenate(outs, axis=0)

    def load_step(t, sums):
        at = pl.ds(pl.multiple_of(t * LANES, LANES), LANES)
        new = []
        for c in range(comps):
            value = gather(warm_ref[c, :, at])
            field[t, c * points : (c + 1) * points] = value
            new.append(sums[c] + value)
        lamb[t] = gather(lame_ref[:, at]) - REF_MODULUS
        shear[t] = gather(shear_ref[:, at]) * 2.0 - 2.0 * REF_MODULUS
        return tuple(new)

    zero = jnp.zeros((points, LANES), F32)
    sums = lax.fori_loop(0, tiles, load_step, (zero,) * comps)
    shift = [
        jnp.broadcast_to(
            macro_cols[c] - jnp.sum(sums[c], axis=1, keepdims=True) * (1.0 / voxels),
            (points, LANES),
        )
        for c in range(comps)
    ]
    macro = jnp.concatenate(
        [jnp.broadcast_to(col, (points, LANES)) for col in macro_cols], axis=0
    )
    group_rows = 16
    groups = rows // group_rows

    def tau_stage(first):
        def step(t, carry):
            eps = []
            for c in range(comps):
                at = slice(c * points, (c + 1) * points)
                value = field[t, at]
                if first:
                    value = value + shift[c]
                    field[t, at] = value
                eps.append(value)
            extra = lamb[t] * (eps[0] + eps[1] + eps[2])
            mu = shear[t]
            for c in range(comps):
                value = mu * eps[c]
                tau[t, c * points : (c + 1) * points] = value + extra if c < 3 else value
            return carry

        lax.fori_loop(0, tiles, step, 0)

    def forward_step(g, carry):
        at = pl.ds(pl.multiple_of(g * group_rows, group_rows), group_rows)
        for parity in (0, 1):
            values = []
            for x in range(side):
                a, b = tau[2 * x, at], tau[2 * x + 1, at]
                values.append(a + b if parity == 0 else a - b)
            out = real_transform(values)
            for s in range(slabs):
                re, im = out[s] if s else (out[0][0], out[slabs][0])
                for k, v in ((0, re), (1, im)):
                    hi, lo = split_rows(v)
                    high[parity, s, at, k * LANES : (k + 1) * LANES] = hi
                    low[parity, s, at, k * LANES : (k + 1) * LANES] = lo
        return carry

    def multiply(th_ref, tl_ref):
        for parity in (0, 1):
            spec[parity, 0] = product(
                high[parity, 0], low[parity, 0], th_ref[parity, 0], tl_ref[parity, 0]
            )
            spec[parity, 1:] = product(
                high[parity, 1:].reshape((slabs - 1) * rows, plane),
                low[parity, 1:].reshape((slabs - 1) * rows, plane),
                th_ref[parity, 1], tl_ref[parity, 1],
            ).reshape(slabs - 1, rows, plane)

    def green_step(index, carry):
        parity = index // slabs
        s = index - parity * slabs
        for k in (0, 1):
            lanes = slice(k * LANES, (k + 1) * LANES)
            table = [
                jnp.broadcast_to(normals_ref[parity, s, k, d : d + 1, :], (8, LANES))
                for d in range(6)
            ]
            results = [[] for _ in range(comps)]
            for o in range(octets):
                entries = [
                    spec[parity, s, c * points + 8 * o : c * points + 8 * o + 8, lanes]
                    for c in range(comps)
                ]
                plus = green(entries, table[0:3])
                minus = green(entries, table[3:6])
                for c in range(comps):
                    value = plus[c] + minus[c]
                    results[c].append(value if c < 3 else value * 0.5)
            for c in range(comps):
                hi, lo = split_rows(jnp.concatenate(results[c], axis=0))
                high[parity, s, c * points : (c + 1) * points, lanes] = hi
                low[parity, s, c * points : (c + 1) * points, lanes] = lo
        return carry

    def inverse_stage(sweep_index):
        for g in range(groups):
            at = slice(g * group_rows, (g + 1) * group_rows)
            base = macro[at]
            mask = jnp.broadcast_to(count_col > float(sweep_index), (points, LANES))
            for yhi in (0, 1):
                parts_k = []
                for s in range(slabs):
                    both = []
                    for k in (0, 1):
                        lanes = slice(k * LANES, (k + 1) * LANES)
                        e, o = spec[0, s, at, lanes], spec[1, s, at, lanes]
                        both.append(e + o if yhi == 0 else e - o)
                    parts_k.append(both)
                spectrum = [(parts_k[0][0], None)] + [tuple(b) for b in parts_k[1:]]
                spectrum.append((parts_k[0][1], None))
                for x, v in enumerate(real_inverse(spectrum)):
                    tile = 2 * x + yhi
                    field[tile, at] = jnp.where(mask, base - v, field[tile, at])

    for sweep_index in (0, 1):
        tau_stage(sweep_index == 0)
        lax.fori_loop(0, groups, forward_step, 0)
        multiply(fh_ref, fl_ref)
        lax.fori_loop(0, 2 * slabs, green_step, 0)
        multiply(ih_ref, il_ref)
        inverse_stage(sweep_index)

    per_owner = points // owners if dense else points

    def stress_step(t, acc):
        eps = [field[t, c * points : (c + 1) * points] for c in range(comps)]
        extra = (lamb[t] + REF_MODULUS) * (eps[0] + eps[1] + eps[2])
        mu = shear[t] + 2.0 * REF_MODULUS
        new = [acc[0] + extra] + [acc[c + 1] + mu * eps[c] for c in range(comps)]
        for c in range(comps):
            if dense:
                for j in range(per_owner):
                    start = (j * comps + c) * tiles + t
                    send_ref[pl.ds(start, owners, stride=per_owner * comps * tiles), :] = (
                        eps[c][j * owners : (j + 1) * owners]
                    )
            else:
                send_ref[c, :, pl.ds(pl.multiple_of(t * LANES, LANES), LANES)] = eps[c]
        return tuple(new)

    acc = lax.fori_loop(0, tiles, stress_step, (zero,) * (comps + 1))
    mean = [jnp.sum(a, axis=1, keepdims=True) * (1.0 / voxels) for a in acc]
    stress_cols = [mean[c + 1] + mean[0] if c < 3 else mean[c + 1] for c in range(comps)]
    stress_rows = [
        jnp.sum(choose * col, axis=0, keepdims=True) for col in stress_cols
    ]
    for c in range(comps):
        stress_ref[c : c + 1, :] = stress_rows[c]

    index_of = ((0, 5, 4), (5, 1, 3), (4, 3, 2))
    weighted = [row * weight_row for row in stress_rows]
    loads = jnp.zeros((nlinks, LANES), F32)
    for i in range(3):
        total = sum(grads[j] * weighted[index_of[i][j]] for j in range(3))
        columns = [
            jnp.sum(jnp.where(glane // 8 == e, total, 0.0), axis=1, keepdims=True)
            for e in range(elements)
        ]
        loads = jnp.where(group == i, jnp.concatenate(columns, axis=0), loads)
    loads = loads * inside
    force_ref[...] = lax.dot_general(
        hit, loads, (((0,), (0,)), ((), ())), preferred_element_type=F32,
        precision=lax.Precision.HIGHEST,
    )


def unpack_kernel(dims, recv_ref, out_ref):
    points, comps, tiles = dims

    def step(t, carry):
        at = pl.ds(pl.multiple_of(t * LANES, LANES), LANES)
        for c in range(comps):
            for h in range(points // 8):
                start = 8 * h * comps * tiles + c * tiles + t
                out_ref[c, 8 * h : 8 * h + 8, at] = recv_ref[
                    pl.ds(start, 8, stride=comps * tiles), :
                ]
        return carry

    lax.fori_loop(0, tiles, step, 0)


def on_device(
    displacement, shape_grads, point_weights, conn, halo_nodes, warm_strain, moduli, owner, sweeps
):
    axes = ("mesh", "rve")
    points, comps, voxels = warm_strain.shape
    side = round(voxels ** (1.0 / 3.0))
    tiles = voxels // LANES
    owners = lax.axis_size("rve")
    devices = lax.axis_size("mesh") * owners
    node_dev = displacement.shape[1]
    nodes_part = node_dev * owners
    halo = halo_nodes.shape[1]
    per_owner = max(2, points // owners)
    dense = per_owner * owners == points and owners == 8
    wide = -(-(nodes_part + 2 * halo) // LANES) * LANES

    row = jnp.zeros((wide,), F32)
    row = row.at[: 3 * node_dev].set(displacement.reshape(-1))
    row = row.at[nodes_part : nodes_part + halo].set(halo_nodes[1].astype(F32))
    row = row.at[nodes_part + halo : nodes_part + 2 * halo].set(halo_nodes[0].astype(F32))
    table = lax.all_to_all(
        jnp.broadcast_to(row[None], (devices, wide)), axes, split_axis=0, concat_axis=0, tiled=True
    )

    ids = jnp.stack([owner.astype(F32), sweeps.astype(F32), point_weights])
    ids = jnp.pad(ids, ((0, 5), (0, LANES - points)))
    elements = conn.shape[1]
    links = jnp.broadcast_to(conn.T.reshape(-1, 1), (8 * elements, wide))
    grads = jnp.pad(shape_grads, ((0, 0), (0, 0), (0, LANES - points)))
    part = lax.axis_index("mesh").astype(jnp.int32).reshape(1)
    warm = warm_strain.transpose(1, 0, 2)
    lame, shear = moduli[:, 0], moduli[:, 1]
    fh, fl, ih, il, normals = build_tables(side)
    dims = (points, comps, side, devices, node_dev, halo, owners, nodes_part, owners, dense)
    rows = comps * points
    plane = side * side
    vmem = pl.BlockSpec(memory_space=pltpu.VMEM)
    if dense:
        send_shape = (points * comps * tiles, LANES)
    else:
        send_shape = (comps, points, voxels)
    send, stress, force = pl.pallas_call(
        functools.partial(main_kernel, dims),
        out_shape=(
            jax.ShapeDtypeStruct(send_shape, F32),
            jax.ShapeDtypeStruct((8, LANES), F32),
            jax.ShapeDtypeStruct((devices, LANES), F32),
        ),
        in_specs=[pl.BlockSpec(memory_space=pltpu.SMEM)] + [vmem] * 12,
        out_specs=(vmem, vmem, vmem),
        scratch_shapes=[
            pltpu.VMEM((tiles, rows, LANES), F32),
            pltpu.VMEM((tiles, rows, LANES), F32),
            pltpu.VMEM((tiles, points, LANES), F32),
            pltpu.VMEM((tiles, points, LANES), F32),
            pltpu.VMEM((2, side // 2, rows, plane), BF16),
            pltpu.VMEM((2, side // 2, rows, plane), BF16),
            pltpu.VMEM((2, side // 2, rows, plane), F32),
        ],
        compiler_params=pltpu.CompilerParams(vmem_limit_bytes=48 << 20),
        name="relax",
    )(part, ids, links, grads, table, warm, lame, shear, fh, fl, ih, il, normals)

    comps_out = stress[:comps, :points]
    pieces = lax.all_to_all(force, axes, split_axis=0, concat_axis=0, tiled=True)
    nodal = jnp.sum(pieces, axis=0)[: 3 * node_dev].reshape(3, node_dev)
    if dense:
        received = lax.all_to_all(send, "rve", split_axis=0, concat_axis=0, tiled=True)
        micro = pl.pallas_call(
            functools.partial(unpack_kernel, (points, comps, tiles)),
            out_shape=jax.ShapeDtypeStruct((comps, points, voxels), F32),
            in_specs=[vmem],
            out_specs=vmem,
            compiler_params=pltpu.CompilerParams(vmem_limit_bytes=16 << 20),
            name="unpack",
        )(received).transpose(1, 0, 2)
    else:
        slots = owners * per_owner
        final = send.transpose(1, 0, 2)
        order = jnp.arange(points, dtype=jnp.int32)
        same = owner[:, None] == owner[None, :]
        rank = jnp.sum((same & (order[None, :] < order[:, None])).astype(jnp.int32), axis=1)
        slot = owner * per_owner + rank
        fields = jnp.zeros((slots, comps, voxels), F32).at[slot].set(final)
        flags = jnp.zeros((slots,), F32).at[slot].set(1.0)
        fields = lax.all_to_all(fields, "rve", split_axis=0, concat_axis=0, tiled=True)
        flags = lax.all_to_all(flags, "rve", split_axis=0, concat_axis=0, tiled=True)
        filled = jnp.nonzero(flags > 0.5, size=points)[0].astype(jnp.int32)
        micro = fields[filled]
    return (nodal, comps_out, micro)


def solution(mesh):
    both = ("mesh", "rve")
    in_specs = (
        P(None, both), P(None, None, both), P(both), P(None, both), P(None, "mesh"),
        P(both, None, None), P(both, None, None), P(both), P(both),
    )
    out_specs = (P(None, both), P(None, both), P(both, None, None))
    return jax.shard_map(
        on_device, mesh=mesh, in_specs=in_specs, out_specs=out_specs, check_vma=False
    )
```

```python
import functools
import math

import jax
import jax.numpy as jnp
import numpy as np
from jax import lax
from jax.experimental import pallas as pl
from jax.experimental.pallas import tpu as pltpu
from jax.sharding import PartitionSpec as P


REF_MODULUS = 1.1
COUPLING = 2.2 / (1.1 * 3.3)
PAIRS = ((0, 0), (1, 1), (2, 2), (1, 2), (0, 2), (0, 1))
F32 = jnp.float32
BF16 = jnp.bfloat16
LANES = 128
WINDOW = 32
SPLIT = 24
PREV_LANE = 16
NEXT_LANE = 32


def signed_waves(side):
    wave = np.arange(side)
    return np.where(wave < side // 2, wave, wave - side)


def normal_at(kx, ky, kz, side):
    signed = signed_waves(side)
    xi = np.stack([signed[kx % side], signed[ky % side], signed[kz % side]]).astype(np.float64)
    length = np.sqrt((xi * xi).sum(0))
    return np.where(length > 0, xi / np.where(length > 0, length, 1.0), 0.0)


def plane_sets(side):
    packs = []
    for parity in (0, 1):
        columns, seen = [], set()
        for ky in range(parity, side, 2):
            for kz in range(side):
                if (ky, kz) in seen:
                    continue
                mirror = (-ky % side, -kz % side)
                seen.update({(ky, kz), mirror})
                if mirror == (ky, kz):
                    columns.append((ky, kz, 0, 1))
                else:
                    columns += [(ky, kz, 0, 0), (ky, kz, 1, 0)]
        packs.append(np.array(columns))
    return packs


def window_order(parity, at_edge):
    edge, rest = list(np.flatnonzero(at_edge)), list(np.flatnonzero(~at_edge))
    lead = SPLIT if parity else 0
    limit = WINDOW - SPLIT if parity else SPLIT
    assert len(edge) <= limit
    return np.array(rest[:lead] + edge + rest[lead:])


def split_table(table):
    high = np.asarray(table, np.float32).astype(jnp.bfloat16)
    low = (np.asarray(table, np.float64) - high.astype(np.float64)).astype(jnp.bfloat16)
    return high, low


def build_tables(side):
    plane = side * side
    half = plane // 2
    edge = side // 2
    ylo, zz = np.divmod(np.arange(half), side)
    scale = 1.0 / (2.2 * side**3)
    forward = np.zeros((2, 2, plane, plane))
    inverse = np.zeros((2, 2, plane, plane))
    tables = np.zeros((2, side // 2, 2, 8, half))
    packs = plane_sets(side)
    for parity in (0, 1):
        kyi, kz = np.divmod(np.arange(half), side)
        ky = 2 * kyi + parity
        order = window_order(parity, (ky == edge) | (kz == edge))
        ky, kz = ky[order], kz[order]
        angle = 2 * np.pi / side * ((np.outer(ylo, ky) + np.outer(zz, kz)) % side)
        c, s = np.cos(angle), np.sin(angle)
        forward[parity, 1] = np.block([[c, -s], [s, c]])
        inverse[parity, 1] = np.block([[c.T, s.T], [-s.T, c.T]]) * scale
        for kx in range(1, side // 2):
            tables[parity, kx, :, 0:3] = normal_at(np.full(half, kx), ky, kz, side)
            tables[parity, kx, :, 3:6] = normal_at(np.full(half, -kx), -ky, -kz, side)
            tables[parity, kx, :, 6] = 2.0
        columns = packs[parity]
        order = window_order(parity, (columns[:, 0] == edge) | (columns[:, 1] == edge))
        ky, kz, imag, single = columns[order].T
        angle = 2 * np.pi / side * ((np.outer(ylo, ky) + np.outer(zz, kz)) % side)
        fwd = np.where(imag[None], -np.sin(angle), np.cos(angle))
        share = np.where(single, 1.0, 2.0)
        inv = (fwd * share[None]).T * scale
        forward[parity, 0, :half, :half] = fwd
        forward[parity, 0, half:, half:] = fwd
        inverse[parity, 0, :half, :half] = inv
        inverse[parity, 0, half:, half:] = inv
        for part, kx in ((0, 0), (1, edge)):
            full = np.full(half, kx)
            tables[parity, 0, part, 0:3] = normal_at(full, ky, kz, side)
            tables[parity, 0, part, 3:6] = normal_at(-full, -ky, -kz, side)
            tables[parity, 0, part, 6] = share
    fh, fl = split_table(forward)
    ih, il = split_table(inverse)
    return np.stack([fh, fl]), np.stack([ih, il]), tables.astype(np.float32)


def real_transform(values):
    count = len(values)
    if count == 2:
        return [(values[0] + values[1], None), (values[0] - values[1], None)]
    even = real_transform(values[0::2])
    odd = real_transform(values[1::2])
    half = count // 2
    result = [None] * (half + 1)
    result[0] = (even[0][0] + odd[0][0], None)
    result[half] = (even[0][0] - odd[0][0], None)
    for k in range(1, half // 2):
        (er, ei), (orr, oi) = even[k], odd[k]
        angle = 2 * math.pi * k / count
        c, s = math.cos(angle), math.sin(angle)
        if abs(c - s) < 1e-9:
            tr, ti = (orr + oi) * c, (oi - orr) * c
        else:
            tr, ti = orr * c + oi * s, oi * c - orr * s
        result[k] = (er + tr, ei + ti)
        result[half - k] = (er - tr, ti - ei)
    result[half // 2] = (even[half // 2][0], -odd[half // 2][0])
    return result


def real_inverse(spectrum):
    half = len(spectrum) - 1
    count = 2 * half
    if count == 2:
        return [spectrum[0][0] + spectrum[1][0], spectrum[0][0] - spectrum[1][0]]
    even = [None] * (half // 2 + 1)
    odd = [None] * (half // 2 + 1)
    even[0] = (spectrum[0][0] + spectrum[half][0], None)
    odd[0] = (spectrum[0][0] - spectrum[half][0], None)
    for k in range(1, half // 2):
        (ar, ai), (br, bi) = spectrum[k], spectrum[half - k]
        even[k] = (ar + br, ai - bi)
        dr, di = ar - br, ai + bi
        angle = 2 * math.pi * k / count
        c, s = math.cos(angle), math.sin(angle)
        if abs(c - s) < 1e-9:
            odd[k] = ((dr - di) * c, (dr + di) * c)
        else:
            odd[k] = (dr * c - di * s, dr * s + di * c)
    mid_re, mid_im = spectrum[half // 2]
    even[half // 2] = (mid_re * 2.0, None)
    odd[half // 2] = (mid_im * -2.0, None)
    first, second = real_inverse(even), real_inverse(odd)
    result = []
    for a, b in zip(first, second):
        result += [a, b]
    return result


def potential(entries, normal):
    n0, n1, n2 = normal
    t0 = entries[0] * n0 + entries[5] * n1 + entries[4] * n2
    t1 = entries[5] * n0 + entries[1] * n1 + entries[3] * n2
    t2 = entries[4] * n0 + entries[3] * n1 + entries[2] * n2
    load = (n0 * t0 + n1 * t1 + n2 * t2) * (COUPLING * 1.1)
    return t0 - n0 * load, t1 - n1 * load, t2 - n2 * load


def strain_of(plus, minus, table):
    n0, n1, n2, m0, m1, m2 = table
    u0, u1, u2 = plus
    v0, v1, v2 = minus
    return (
        n0 * u0 + m0 * v0,
        n1 * u1 + m1 * v1,
        n2 * u2 + m2 * v2,
        (n1 * u2 + n2 * u1 + m1 * v2 + m2 * v1) * 0.5,
        (n0 * u2 + n2 * u0 + m0 * v2 + m2 * v0) * 0.5,
        (n0 * u1 + n1 * u0 + m0 * v1 + m1 * v0) * 0.5,
    )


def split_rows(value):
    high = value.astype(BF16)
    return high, (value - high.astype(F32)).astype(BF16)


def product(high, low, table_high, table_low):
    dot = functools.partial(jnp.dot, preferred_element_type=F32)
    return dot(high, table_high) + (dot(low, table_high) + dot(high, table_low))


def column_to_row(column, diagonal):
    return jnp.sum(jnp.where(diagonal, column, 0.0), axis=0, keepdims=True)


def row_to_column(row, diagonal):
    return jnp.sum(jnp.where(diagonal, row, 0.0), axis=1, keepdims=True)


def padded_row(ref):
    row = ref[...].astype(F32)
    return jnp.concatenate([row, jnp.zeros((1, LANES - row.shape[1]), F32)], axis=1)


def slot_choice(owner_ref, points, owners, dense):
    lane = lax.broadcasted_iota(jnp.int32, (points, LANES), 1)
    sub = lax.broadcasted_iota(jnp.int32, (points, LANES), 0)
    diagonal = lane == sub
    if not dense:
        return jnp.where(diagonal, 1.0, 0.0), lane
    owner_row = padded_row(owner_ref)
    owner_col = row_to_column(owner_row, diagonal)
    earlier = jnp.where((owner_col == owner_row) & (lane < sub), 1.0, 0.0)
    rank_col = jnp.sum(earlier, axis=1, keepdims=True)
    slot_row = column_to_row(rank_col * owners + owner_col, diagonal)
    return jnp.where((slot_row == sub.astype(F32)) & (lane < points), 1.0, 0.0), lane


def forward_groups(dims, groups, tau, high, low):
    side, slabs = dims

    def step(g, carry):
        at = pl.ds(pl.multiple_of(g * 16, 16), 16)
        for parity in (0, 1):
            values = []
            for x in range(side):
                a, b = tau[2 * x, at], tau[2 * x + 1, at]
                values.append(a + b if parity == 0 else a - b)
            out = real_transform(values)
            for s in range(slabs):
                re, im = out[s] if s else (out[0][0], out[slabs][0])
                for k, v in ((0, re), (1, im)):
                    hi, lo = split_rows(v)
                    high[parity, s, at, k * LANES : (k + 1) * LANES] = hi
                    low[parity, s, at, k * LANES : (k + 1) * LANES] = lo
        return carry

    lax.fori_loop(0, groups, step, 0)


def multiply(high, low, table, spec, done=None):
    slabs, rows, plane = high.shape[1:]
    for parity in (0, 1):
        spec[parity, 0] = product(
            high[parity, 0], low[parity, 0], table[0, parity, 0], table[1, parity, 0]
        )
        spec[parity, 1:] = product(
            high[parity, 1:].reshape((slabs - 1) * rows, plane),
            low[parity, 1:].reshape((slabs - 1) * rows, plane),
            table[0, parity, 1], table[1, parity, 1],
        ).reshape(slabs - 1, rows, plane)
        if done is not None:
            done(parity)


def inverse_rows(spec, at, slabs, emit):
    for yhi in (0, 1):
        parts = []
        for s in range(slabs):
            both = []
            for k in (0, 1):
                lanes = slice(k * LANES, (k + 1) * LANES)
                e, o = spec[0, s, at, lanes], spec[1, s, at, lanes]
                both.append(e + o if yhi == 0 else e - o)
            parts.append(both)
        spectrum = [(parts[0][0], None)] + [tuple(b) for b in parts[1:]]
        spectrum.append((parts[0][1], None))
        for x, v in enumerate(real_inverse(spectrum)):
            emit(2 * x + yhi, v)


def first_kernel(
    dims, owner_ref, warm_hbm, moduli_hbm, forward_hbm,
    spec_hbm, both_hbm, mean_ref,
    forward, warm, moduli, spec, tau, high, low, sems,
):
    points, comps, side, owners, dense = dims
    tiles = side**3 // LANES
    parts = 4
    span = side**3 // parts
    stride = moduli.shape[0] // points
    moduli_copies = [
        pltpu.make_async_copy(
            moduli_hbm.at[g], moduli.at[pl.ds(g * stride, 2 * tiles)], sems.at[0]
        )
        for g in range(points)
    ]
    warm_copies = [
        pltpu.make_async_copy(
            warm_hbm.at[:, :, pl.ds(q * span, span)], warm.at[:, :, pl.ds(q * span, span)],
            sems.at[1 + q],
        )
        for q in range(parts)
    ]
    table_copy = pltpu.make_async_copy(forward_hbm, forward, sems.at[1 + parts])
    for copy in moduli_copies + warm_copies + [table_copy]:
        copy.start()
    octets = points // 8
    choose, lane = slot_choice(owner_ref, points, owners, dense)
    pick = jnp.sum(choose * lane.astype(F32), axis=1, keepdims=True).astype(jnp.int32)
    picks = [jnp.broadcast_to(pick[8 * o : 8 * o + 8], (8, LANES)) for o in range(octets)]
    locals_ = [
        [jnp.clip(picks[o] - 8 * source, 0, 7) for source in range(octets)] for o in range(octets)
    ]
    beyond = [[picks[o] >= 8 * source for source in range(octets)] for o in range(octets)]

    def gather(value):
        if not dense:
            return value
        outs = []
        for o in range(octets):
            best = None
            for source in range(octets):
                got = jnp.take_along_axis(
                    value[8 * source : 8 * source + 8], locals_[o][source], axis=0,
                    mode="promise_in_bounds",
                )
                best = got if best is None else jnp.where(beyond[o][source], got, best)
            outs.append(best)
        return jnp.concatenate(outs, axis=0)

    def load_step(t, sums):
        at = pl.ds(pl.multiple_of(t * LANES, LANES), LANES)
        pair = [
            gather(
                jnp.concatenate(
                    [
                        moduli[pl.ds(8 * o * stride + 2 * t + i, 8, stride=stride), :]
                        for o in range(octets)
                    ],
                    axis=0,
                )
            )
            for i in (0, 1)
        ]
        lamb = pair[0] - REF_MODULUS
        mu = pair[1] * 2.0 - 2.0 * REF_MODULUS
        eps = [gather(warm[c, :, at]) for c in range(comps)]
        extra = lamb * (eps[0] + eps[1] + eps[2])
        for c in range(comps):
            value = mu * eps[c]
            tau[t, c * points : (c + 1) * points] = value + extra if c < 3 else value
        tau[t, comps * points : (comps + 1) * points] = lamb
        tau[t, (comps + 1) * points :] = mu
        return tuple(s + e for s, e in zip(sums, eps + [lamb, mu]))

    zero = jnp.zeros((points, LANES), F32)
    sums = (zero,) * (comps + 2)
    for copy in moduli_copies:
        copy.wait()
    for q in range(parts):
        warm_copies[q].wait()
        sums = lax.fori_loop(q * tiles // parts, (q + 1) * tiles // parts, load_step, sums)
    both_copy = pltpu.make_async_copy(
        tau.at[:, pl.ds(comps * points, 2 * points)], both_hbm, sems.at[0]
    )
    both_copy.start()
    for c in range(comps + 2):
        mean_ref[c * points : (c + 1) * points] = jnp.broadcast_to(
            jnp.sum(sums[c], axis=1, keepdims=True) * (1.0 / side**3), (points, LANES)
        )
    forward_groups((side, side // 2), (comps + 2) * points // 16, tau, high, low)
    table_copy.wait()
    out_copies = []

    def done(parity):
        copy = pltpu.make_async_copy(spec.at[parity], spec_hbm.at[parity], sems.at[1 + parity])
        copy.start()
        out_copies.append(copy)

    multiply(high, low, forward, spec, done)
    both_copy.wait()
    for copy in out_copies:
        copy.wait()


def second_kernel(
    dims,
    part_ref, owner_ref, sweeps_ref, weight_ref, conn_ref, grads_ref, table_ref, mean_ref,
    normals_ref, first_hbm, both_hbm, forward_hbm, inverse_hbm,
    send_ref, stress_ref, force_ref,
    first_ref, both, forward, inverse, tau, high, low, spec, pot, edge, full, macro_buf, loads_buf,
    sems, slab_sems,
):
    points, comps, side, devices, node_dev, halo, row_span, nodes_part, owners, dense = dims
    copies = [
        pltpu.make_async_copy(inverse_hbm, inverse, sems.at[0]),
        pltpu.make_async_copy(both_hbm, both, sems.at[1]),
        pltpu.make_async_copy(forward_hbm, forward, sems.at[2]),
    ]

    def slab_copy(s):
        return pltpu.make_async_copy(
            first_hbm.at[:, pl.ds(s, 1)], first_ref.at[:, pl.ds(s, 1)], slab_sems.at[s]
        )

    for s in range(side // 2):
        slab_copy(s).start()
    for copy in copies:
        copy.start()
    voxels = side**3
    tiles = voxels // LANES
    slabs = side // 2
    part = part_ref[0]
    choose, _ = slot_choice(owner_ref, points, owners, dense)
    count_col = jnp.sum(choose * padded_row(sweeps_ref), axis=1, keepdims=True)
    weight_row = padded_row(weight_ref)

    exch = table_ref[...]
    dev_sub = lax.broadcasted_iota(jnp.int32, exch.shape, 0)
    below = jnp.sum(jnp.where(dev_sub == (part - 1) * row_span, exch, 0.0), axis=0, keepdims=True)
    above = jnp.sum(jnp.where(dev_sub == (part + 1) * row_span, exch, 0.0), axis=0, keepdims=True)
    parts = devices // row_span
    wide = table_ref.shape[1]
    elane = lax.broadcasted_iota(jnp.int32, (1, wide), 1)
    lane_f = elane.astype(F32)
    part_f = part.astype(F32)
    span = float(nodes_part)
    low_id = jnp.where(part > 0, below + (part_f - 1.0) * span, -1.0)
    high_id = jnp.where(part < parts - 1, above + (part_f + 1.0) * span, -1.0)
    node_row = jnp.where(
        elane < nodes_part,
        part_f * span + lane_f,
        jnp.where(elane < nodes_part + halo, low_id, high_id),
    )
    corner = lax.broadcasted_iota(jnp.int32, (8, LANES), 0)
    corner_lane = lax.broadcasted_iota(jnp.int32, (8, LANES), 1)
    link_rows = conn_ref[...].astype(F32)
    link_rows = jnp.concatenate(
        [link_rows, jnp.zeros((link_rows.shape[0], LANES - 8), F32)], axis=1
    )
    links = jnp.concatenate(
        [row_to_column(link_rows[e : e + 1], corner == corner_lane) for e in range(points // 8)],
        axis=0,
    )
    node_col = jnp.sum(jnp.where(links == lane_f, node_row, 0.0), axis=1, keepdims=True)
    device_col = jnp.floor(node_col * (1.0 / node_dev))
    inner_col = node_col - device_col * node_dev
    nlinks = links.shape[0]
    hit_lane = lax.broadcasted_iota(jnp.int32, (nlinks, devices), 1).astype(F32)
    hit = jnp.where(hit_lane == device_col, 1.0, 0.0)
    flat_lane = lax.broadcasted_iota(jnp.int32, (nlinks, LANES), 1)
    group = flat_lane // node_dev
    inside = jnp.where(
        ((flat_lane - group * node_dev).astype(F32) == inner_col) & (group < 3), 1.0, 0.0
    )
    fetched = jnp.dot(hit, exch[:, :LANES], preferred_element_type=F32,
                      precision=lax.Precision.HIGHEST) * inside
    moved = [
        jnp.sum(jnp.where(group == i, fetched, 0.0), axis=1, keepdims=True) for i in range(3)
    ]
    elements = points // 8
    glane = lax.broadcasted_iota(jnp.int32, (8, LANES), 1)
    spread = []
    for i in range(3):
        acc = jnp.zeros((8, LANES), F32)
        for e in range(elements):
            acc = jnp.where(glane // 8 == e, moved[i][8 * e : 8 * e + 8], acc)
        spread.append(acc)
    grads = [
        jnp.concatenate([grads_ref[j], jnp.zeros((8, LANES - points), F32)], axis=1)
        for j in range(3)
    ]
    grad = [
        [jnp.sum(spread[i] * grads[j], axis=0, keepdims=True) for j in range(3)] for i in range(3)
    ]
    macro_rows = [grad[0][0], grad[1][1], grad[2][2]] + [
        (grad[a][b] + grad[b][a]) * 0.5 for a, b in PAIRS[3:]
    ]
    macro_cols = [jnp.sum(choose * row, axis=1, keepdims=True) for row in macro_rows]


    octets = points // 8
    shift = [
        jnp.broadcast_to(macro_cols[c], (points, LANES)) - mean_ref[c * points : (c + 1) * points]
        for c in range(comps)
    ]
    shift_trace = shift[0] + shift[1] + shift[2]
    macro = [jnp.broadcast_to(col, (points, LANES)) for col in macro_cols]
    again = jnp.broadcast_to(count_col > 1.0, (points, LANES))
    block = send_ref.shape[0] // points

    def send(o, index, value):
        if dense:
            per_owner = points // owners
            send_ref[pl.ds(o * block + index, owners, stride=per_owner * block), :] = value
        else:
            send_ref[pl.ds(8 * o * block + index, 8, stride=block), :] = value

    edge_base = 3 * 4 * slabs
    window_rows = slabs * 2 * WINDOW // LANES
    at_window = lax.broadcasted_iota(jnp.int32, (8, LANES), 1)

    def green_stage(last):
        def load(parity, s, k, o):
            lanes = slice(k * LANES, (k + 1) * LANES)
            if last:
                return [
                    spec[parity, s, c * points + 8 * o : c * points + 8 * o + 8, lanes]
                    for c in range(comps)
                ]
            rows = slice(8 * o, 8 * o + 8)
            raw = [
                first_ref[parity, s, c * points + 8 * o : c * points + 8 * o + 8, lanes]
                for c in range(comps + 2)
            ]
            extra = raw[comps] * shift_trace[rows]
            entries = [raw[c] + raw[comps + 1] * shift[c][rows] for c in range(comps)]
            return [entries[c] + extra if c < 3 else entries[c] for c in range(comps)]

        def step(s, acc):
            acc = list(acc)
            if not last:
                slab_copy(s).wait()
            for k in (0, 1):
                lanes = slice(k * LANES, (k + 1) * LANES)
                results = [[[] for _ in range(comps)] for _ in (0, 1)]
                edges = [[None, None] for _ in range(octets)]
                for parity in (0, 1):
                    table = [
                        jnp.broadcast_to(normals_ref[parity, s, k, d : d + 1, :], (8, LANES))
                        for d in range(7)
                    ]
                    for o in range(octets):
                        rows = slice(8 * o, 8 * o + 8)
                        entries = load(parity, s, k, o)
                        plus = potential(entries, table[0:3])
                        minus = potential(entries, table[3:6])
                        strains = strain_of(plus, minus, table[0:6])
                        for c in range(comps):
                            results[parity][c].append(strains[c])
                        share_l = table[6] * first_ref[
                            parity, s, comps * points + 8 * o : comps * points + 8 * o + 8, lanes
                        ]
                        share_m = table[6] * first_ref[
                            parity, s,
                            (comps + 1) * points + 8 * o : (comps + 1) * points + 8 * o + 8, lanes,
                        ]
                        base = o * (comps + 1)
                        acc[base] = acc[base] + share_l * (strains[0] + strains[1] + strains[2])
                        for c in range(comps):
                            acc[base + 1 + c] = acc[base + 1 + c] + share_m * strains[c]
                        edges[o][parity] = minus
                        for d in range(3):
                            index = (d * 2 + parity) * slabs * 2 + s * 2 + k
                            if last:
                                kept = pot[o, index]
                                send(o, index, jnp.where(again[rows], plus[d], kept))
                            else:
                                pot[o, index] = plus[d]
                if not last:
                    for parity in (0, 1):
                        for c in range(comps):
                            hi, lo = split_rows(jnp.concatenate(results[parity][c], axis=0))
                            high[parity, s, c * points : (c + 1) * points, lanes] = hi
                            low[parity, s, c * points : (c + 1) * points, lanes] = lo
                for o in range(octets):
                    for d in range(3):
                        joined = jnp.where(
                            at_window < SPLIT, edges[o][0][d], edges[o][1][d]
                        )
                        edge[o, d, s * 2 + k] = (
                            jnp.where(again[8 * o : 8 * o + 8], joined, edge[o, d, s * 2 + k])
                            if last else joined
                        )
                        if k == 1:
                            @pl.when(s == 0)
                            def _():
                                for parity in (0, 1):
                                    value = edges[o][parity][d]
                                    if last:
                                        value = jnp.where(
                                            again[8 * o : 8 * o + 8], value, full[o, d, parity]
                                        )
                                    full[o, d, parity] = value
            return tuple(acc)

        zero = jnp.zeros((8, LANES), F32)
        return lax.fori_loop(0, slabs, step, (zero,) * (octets * (comps + 1)))

    first = green_stage(False)
    copies[0].wait()
    multiply(high, low, inverse, spec)

    def field_step(c, carry):
        at = pl.ds(pl.multiple_of(c * points, points), points)
        base = macro_buf[c]

        def emit(tile, value):
            tau[tile, at] = base - value

        inverse_rows(spec, at, slabs, emit)
        return carry

    for c in range(comps):
        macro_buf[c] = macro[c]
    lax.fori_loop(0, comps, field_step, 0)
    copies[1].wait()

    def tau_step(t, carry):
        eps = [tau[t, c * points : (c + 1) * points] for c in range(comps)]
        extra = both[t, :points] * (eps[0] + eps[1] + eps[2])
        mu = both[t, points:]
        for c in range(comps):
            value = mu * eps[c]
            tau[t, c * points : (c + 1) * points] = value + extra if c < 3 else value
        return carry

    lax.fori_loop(0, tiles, tau_step, 0)
    forward_groups((side, slabs), comps * points // 16, tau, high, low)
    copies[2].wait()
    multiply(high, low, forward, spec)
    second = green_stage(True)

    row_lane = lax.broadcasted_iota(jnp.int32, (8, LANES), 1)
    per_row = LANES // WINDOW
    for o in range(octets):
        for d in range(3):
            for v in range(2 * slabs // per_row):
                value = edge[o, d, v * per_row]
                for q in range(1, per_row):
                    moved_q = pltpu.roll(edge[o, d, v * per_row + q], q * WINDOW, 1)
                    value = jnp.where(row_lane >= q * WINDOW, moved_q, value)
                send(o, edge_base + d * (2 * slabs // per_row) + v, value)
            for parity in (0, 1):
                send(o, edge_base + 3 * window_rows + d * 2 + parity, full[o, d, parity])
        value = jnp.zeros((8, LANES), F32)
        for c in range(comps):
            value = jnp.where(row_lane == c, macro[c][8 * o : 8 * o + 8], value)
        send(o, edge_base + 3 * window_rows + 6, value)

    sums = []
    for q in range(comps + 1):
        rows = [
            jnp.where(
                again[8 * o : 8 * o + 8], second[o * (comps + 1) + q], first[o * (comps + 1) + q]
            )
            for o in range(octets)
        ]
        sums.append(
            jnp.sum(jnp.concatenate(rows, axis=0), axis=1, keepdims=True)
            * (1.0 / (2.2 * float(voxels) * float(voxels)))
        )
    lamb_mean = mean_ref[comps * points : (comps + 1) * points]
    mu_mean = mean_ref[(comps + 1) * points :]
    trace = macro[0] + macro[1] + macro[2]
    bulk = (lamb_mean + REF_MODULUS) * trace - sums[0]
    stress_rows = []
    for c in range(comps):
        value = (mu_mean + 2.0 * REF_MODULUS) * macro[c] - sums[1 + c]
        if c < 3:
            value = value + bulk
        stress_rows.append(jnp.sum(choose * value, axis=0, keepdims=True))
    for c in range(comps):
        stress_ref[c : c + 1, :] = stress_rows[c]

    index_of = ((0, 5, 4), (5, 1, 3), (4, 3, 2))
    weighted = [row * weight_row for row in stress_rows]
    loads = jnp.zeros((nlinks, LANES), F32)
    for i in range(3):
        total = sum(grads[j] * weighted[index_of[i][j]] for j in range(3))
        columns = [
            jnp.sum(jnp.where(glane // 8 == e, total, 0.0), axis=1, keepdims=True)
            for e in range(elements)
        ]
        loads = jnp.where(group == i, jnp.concatenate(columns, axis=0), loads)
    loads = loads * inside
    force = lax.dot_general(
        hit, loads, (((0,), (0,)), ((), ())), preferred_element_type=F32,
        precision=lax.Precision.HIGHEST,
    )
    force_ref[...] = force
    last_row = edge_base + 3 * window_rows + 7
    for o in range(octets):
        send(o, last_row, jnp.zeros((8, LANES), F32))
    if dense:
        loads_buf[...] = jnp.zeros_like(loads_buf)
        loads_buf[row_span : row_span + devices] = force
        near = [
            loads_buf[pl.ds(pl.multiple_of((part + i) * row_span, row_span), row_span), :]
            for i in range(3)
        ]
        send(
            0, last_row,
            near[1] + pltpu.roll(near[0], PREV_LANE, 1) + pltpu.roll(near[2], NEXT_LANE, 1),
        )


def third_kernel(
    dims, recv_ref, normals_ref, inverse_hbm, out_ref, inverse, high, low, spec, sem
):
    points, comps, side = dims
    copy = pltpu.make_async_copy(inverse_hbm, inverse, sem)
    copy.start()
    slabs = side // 2
    block = recv_ref.shape[0] // points
    edge_base = 3 * 4 * slabs
    per_row = LANES // WINDOW
    window_rows = 2 * slabs // per_row
    octets = points // 8
    lane = lax.broadcasted_iota(jnp.int32, (8, LANES), 1)

    def fetch(o, index):
        return recv_ref[pl.ds(8 * o * block + index, 8, stride=block), :]

    for s in range(slabs):
        for k in (0, 1):
            window = s * 2 + k
            lanes = slice(k * LANES, (k + 1) * LANES)
            edges = []
            for o in range(octets):
                row = []
                for d in range(3):
                    value = fetch(o, edge_base + d * window_rows + window // per_row)
                    turn = (window % per_row) * WINDOW
                    row.append(pltpu.roll(value, LANES - turn, 1) if turn else value)
                edges.append(row)
            for parity in (0, 1):
                table = [
                    jnp.broadcast_to(normals_ref[parity, s, k, d : d + 1, :], (8, LANES))
                    for d in range(6)
                ]
                if parity == 0:
                    inside = lane < SPLIT
                else:
                    inside = (lane >= SPLIT) & (lane < WINDOW)
                results = [[] for _ in range(comps)]
                for o in range(octets):
                    plus = [
                        fetch(o, (d * 2 + parity) * slabs * 2 + window) for d in range(3)
                    ]
                    if s == 0 and k == 1:
                        minus = [
                            fetch(o, edge_base + 3 * window_rows + d * 2 + parity)
                            for d in range(3)
                        ]
                    else:
                        minus = [jnp.where(inside, edges[o][d], -plus[d]) for d in range(3)]
                    strains = strain_of(plus, minus, table)
                    for c in range(comps):
                        results[c].append(strains[c])
                for c in range(comps):
                    hi, lo = split_rows(jnp.concatenate(results[c], axis=0))
                    high[parity, s, c * points : (c + 1) * points, lanes] = hi
                    low[parity, s, c * points : (c + 1) * points, lanes] = lo
    copy.wait()
    multiply(high, low, inverse, spec)
    tops = [fetch(o, edge_base + 3 * window_rows + 6) for o in range(octets)]
    for c in range(comps):
        base = jnp.concatenate(
            [jnp.broadcast_to(top[:, c : c + 1], (8, LANES)) for top in tops], axis=0
        )

        def emit(tile, value):
            out_ref[c, :, tile * LANES : (tile + 1) * LANES] = base - value

        inverse_rows(spec, slice(c * points, (c + 1) * points), slabs, emit)


def pack_kernel(dims, displacement_ref, halo_ref, out_ref):
    nodes_part, halo = dims
    moved = displacement_ref[...]
    halo_f = halo_ref[...].astype(F32)
    node_dev = moved.shape[1]
    wide = out_ref.shape[1]
    pieces = [moved[0:1], moved[1:2], moved[2:3]]
    pieces.append(jnp.zeros((1, nodes_part - 3 * node_dev), F32))
    pieces += [halo_f[1:2], halo_f[0:1]]
    pieces.append(jnp.zeros((1, wide - nodes_part - 2 * halo), F32))
    out_ref[...] = jnp.broadcast_to(jnp.concatenate(pieces, axis=1), out_ref.shape)


def on_device(
    displacement, shape_grads, point_weights, conn, halo_nodes, warm_strain, moduli, owner, sweeps
):
    axes = ("mesh", "rve")
    points, comps, voxels = warm_strain.shape
    side = round(voxels ** (1.0 / 3.0))
    tiles = voxels // LANES
    slabs = side // 2
    plane = side * side
    owners = lax.axis_size("rve")
    devices = lax.axis_size("mesh") * owners
    node_dev = displacement.shape[1]
    nodes_part = node_dev * owners
    halo = halo_nodes.shape[1]
    per_owner = max(2, points // owners)
    dense = per_owner * owners == points and owners == 8
    wide = -(-(nodes_part + 2 * halo) // LANES) * LANES
    vmem = pl.BlockSpec(memory_space=pltpu.VMEM)
    hbm = pl.BlockSpec(memory_space=pltpu.HBM)
    params = pltpu.CompilerParams(vmem_limit_bytes=63 << 20)

    packed = pl.pallas_call(
        functools.partial(pack_kernel, (nodes_part, halo)),
        out_shape=jax.ShapeDtypeStruct((devices, wide), F32),
        in_specs=[vmem, vmem],
        out_specs=vmem,
        name="pack",
    )(displacement, halo_nodes)
    table = lax.all_to_all(packed, axes, split_axis=0, concat_axis=0, tiled=True)

    owner_row = owner.reshape(1, points)
    sweeps_row = sweeps.reshape(1, points)
    weight_row = point_weights.reshape(1, points)
    part = lax.axis_index("mesh").astype(jnp.int32).reshape(1)
    warm = warm_strain.transpose(1, 0, 2)
    moduli_rows = (
        moduli.reshape(points, 2, tiles, LANES).transpose(0, 2, 1, 3).reshape(points, -1, LANES)
    )
    forward, inverse, normals = (jnp.asarray(t) for t in build_tables(side))
    rows = comps * points
    more = (comps + 2) * points
    octets = points // 8
    table_scratch = pltpu.VMEM(forward.shape, BF16)
    spec, both, mean = pl.pallas_call(
        functools.partial(first_kernel, (points, comps, side, owners, dense)),
        out_shape=(
            jax.ShapeDtypeStruct((2, slabs, more, plane), F32),
            jax.ShapeDtypeStruct((tiles, 2 * points, LANES), F32),
            jax.ShapeDtypeStruct((more, LANES), F32),
        ),
        in_specs=[vmem, hbm, hbm, hbm],
        out_specs=(hbm, hbm, vmem),
        scratch_shapes=[
            table_scratch,
            pltpu.VMEM((comps, points, voxels), F32),
            pltpu.VMEM((points * (2 * tiles + 8), LANES), F32),
            pltpu.VMEM((2, slabs, more, plane), F32),
            pltpu.VMEM((tiles, more, LANES), F32),
            pltpu.VMEM((2, slabs, more, plane), BF16),
            pltpu.VMEM((2, slabs, more, plane), BF16),
            pltpu.SemaphoreType.DMA((6,)),
        ],
        compiler_params=params,
        cost_estimate=pl.CostEstimate(
            flops=2 * 3 * 16 * more * plane * plane, transcendentals=0, bytes_accessed=4 << 20
        ),
        name="first",
    )(owner_row, warm, moduli_rows, forward)

    dims = (points, comps, side, devices, node_dev, halo, owners, nodes_part, owners, dense)
    block = 3 * 4 * slabs + 3 * (2 * slabs * WINDOW // LANES) + 8
    send, stress, force = pl.pallas_call(
        functools.partial(second_kernel, dims),
        out_shape=(
            jax.ShapeDtypeStruct((points * block, LANES), F32),
            jax.ShapeDtypeStruct((8, LANES), F32),
            jax.ShapeDtypeStruct((devices, LANES), F32),
        ),
        in_specs=[pl.BlockSpec(memory_space=pltpu.SMEM)] + [vmem] * 8 + [hbm] * 4,
        out_specs=(vmem,) * 3,
        scratch_shapes=[
            pltpu.VMEM((2, slabs, more, plane), F32),
            pltpu.VMEM((tiles, 2 * points, LANES), F32),
            table_scratch,
            table_scratch,
            pltpu.VMEM((tiles, rows, LANES), F32),
            pltpu.VMEM((2, slabs, rows, plane), BF16),
            pltpu.VMEM((2, slabs, rows, plane), BF16),
            pltpu.VMEM((2, slabs, rows, plane), F32),
            pltpu.VMEM((octets, 3 * 4 * slabs, 8, LANES), F32),
            pltpu.VMEM((octets, 3, 2 * slabs, 8, LANES), F32),
            pltpu.VMEM((octets, 3, 2, 8, LANES), F32),
            pltpu.VMEM((comps, points, LANES), F32),
            pltpu.VMEM((devices + 2 * owners, LANES), F32),
            pltpu.SemaphoreType.DMA((3,)),
            pltpu.SemaphoreType.DMA((slabs,)),
        ],
        compiler_params=params,
        cost_estimate=pl.CostEstimate(
            flops=2 * 2 * 3 * 16 * rows * plane * plane, transcendentals=0, bytes_accessed=6 << 20
        ),
        name="second",
    )(
        part, owner_row, sweeps_row, weight_row, conn.T, shape_grads, table, mean, normals,
        spec, both, forward, inverse,
    )

    finish = pl.pallas_call(
        functools.partial(third_kernel, (points, comps, side)),
        out_shape=jax.ShapeDtypeStruct((comps, points, voxels), F32),
        in_specs=[vmem, vmem, hbm],
        out_specs=vmem,
        scratch_shapes=[
            table_scratch,
            pltpu.VMEM((2, slabs, rows, plane), BF16),
            pltpu.VMEM((2, slabs, rows, plane), BF16),
            pltpu.VMEM((2, slabs, rows, plane), F32),
            pltpu.SemaphoreType.DMA,
        ],
        compiler_params=pltpu.CompilerParams(vmem_limit_bytes=24 << 20),
        cost_estimate=pl.CostEstimate(
            flops=2 * 3 * 16 * rows * plane * plane, transcendentals=0, bytes_accessed=4 << 20
        ),
        name="third",
    )
    comps_out = stress[:comps, :points]
    if dense:
        received = lax.all_to_all(
            send.reshape(owners, per_owner * block, LANES), "rve",
            split_axis=0, concat_axis=0, tiled=True,
        ).reshape(points * block, LANES)
        micro = finish(received, normals, inverse).transpose(1, 0, 2)
        found = received.reshape(owners, per_owner * block, LANES)[:, block - 1]
        found = jnp.sum(found, axis=0)
        parts = lax.axis_size("mesh")
        up = lax.ppermute(found, "mesh", [(i, i + 1) for i in range(parts - 1)])
        down = lax.ppermute(found, "mesh", [(i + 1, i) for i in range(parts - 1)])
        count = 3 * node_dev
        nodal = (
            found[:count] + up[NEXT_LANE : NEXT_LANE + count] + down[PREV_LANE : PREV_LANE + count]
        ).reshape(3, node_dev)
    else:
        slots = owners * per_owner
        final = finish(send, normals, inverse).transpose(1, 0, 2)
        order = jnp.arange(points, dtype=jnp.int32)
        same = owner[:, None] == owner[None, :]
        rank = jnp.sum((same & (order[None, :] < order[:, None])).astype(jnp.int32), axis=1)
        slot = owner * per_owner + rank
        fields = jnp.zeros((slots, comps, voxels), F32).at[slot].set(final)
        flags = jnp.zeros((slots,), F32).at[slot].set(1.0)
        fields = lax.all_to_all(fields, "rve", split_axis=0, concat_axis=0, tiled=True)
        flags = lax.all_to_all(flags, "rve", split_axis=0, concat_axis=0, tiled=True)
        filled = jnp.nonzero(flags > 0.5, size=points)[0].astype(jnp.int32)
        micro = fields[filled]
        pieces = lax.all_to_all(force, axes, split_axis=0, concat_axis=0, tiled=True)
        nodal = jnp.sum(pieces, axis=0)[: 3 * node_dev].reshape(3, node_dev)
    return (nodal, comps_out, micro)


def solution(mesh):
    both = ("mesh", "rve")
    in_specs = (
        P(None, both), P(None, None, both), P(both), P(None, both), P(None, "mesh"),
        P(both, None, None), P(both, None, None), P(both), P(both),
    )
    out_specs = (P(None, both), P(None, both), P(both, None, None))

    return jax.shard_map(
        on_device, mesh=mesh, in_specs=in_specs, out_specs=out_specs, check_vma=False
    )
```

```python
import functools
import math

import jax
import jax.numpy as jnp
import numpy as np
from jax import lax
from jax.experimental import pallas as pl
from jax.experimental.pallas import tpu as pltpu
from jax.sharding import PartitionSpec as P


REF_MODULUS = 1.1
COUPLING = 2.2 / (1.1 * 3.3)
PAIRS = ((0, 0), (1, 1), (2, 2), (1, 2), (0, 2), (0, 1))
F32 = jnp.float32
BF16 = jnp.bfloat16
LANES = 128
WINDOW = 32
SPLIT = 24


def signed_waves(side):
    wave = np.arange(side)
    return np.where(wave < side // 2, wave, wave - side)


def normal_at(kx, ky, kz, side):
    signed = signed_waves(side)
    xi = np.stack([signed[kx % side], signed[ky % side], signed[kz % side]]).astype(np.float64)
    length = np.sqrt((xi * xi).sum(0))
    return np.where(length > 0, xi / np.where(length > 0, length, 1.0), 0.0)


def plane_sets(side):
    packs = []
    for parity in (0, 1):
        columns, seen = [], set()
        for ky in range(parity, side, 2):
            for kz in range(side):
                if (ky, kz) in seen:
                    continue
                mirror = (-ky % side, -kz % side)
                seen.update({(ky, kz), mirror})
                if mirror == (ky, kz):
                    columns.append((ky, kz, 0, 1))
                else:
                    columns += [(ky, kz, 0, 0), (ky, kz, 1, 0)]
        packs.append(np.array(columns))
    return packs


def window_order(parity, at_edge):
    edge, rest = list(np.flatnonzero(at_edge)), list(np.flatnonzero(~at_edge))
    lead = SPLIT if parity else 0
    limit = WINDOW - SPLIT if parity else SPLIT
    assert len(edge) <= limit
    return np.array(rest[:lead] + edge + rest[lead:])


def split_table(table):
    high = np.asarray(table, np.float32).astype(jnp.bfloat16)
    low = (np.asarray(table, np.float64) - high.astype(np.float64)).astype(jnp.bfloat16)
    return high, low


def build_tables(side):
    plane = side * side
    half = plane // 2
    edge = side // 2
    ylo, zz = np.divmod(np.arange(half), side)
    scale = 1.0 / (2.2 * side**3)
    forward = np.zeros((2, 2, plane, plane))
    inverse = np.zeros((2, 2, plane, plane))
    tables = np.zeros((2, side // 2, 2, 8, half))
    packs = plane_sets(side)
    for parity in (0, 1):
        kyi, kz = np.divmod(np.arange(half), side)
        ky = 2 * kyi + parity
        order = window_order(parity, (ky == edge) | (kz == edge))
        ky, kz = ky[order], kz[order]
        angle = 2 * np.pi / side * ((np.outer(ylo, ky) + np.outer(zz, kz)) % side)
        c, s = np.cos(angle), np.sin(angle)
        forward[parity, 1] = np.block([[c, -s], [s, c]])
        inverse[parity, 1] = np.block([[c.T, s.T], [-s.T, c.T]]) * scale
        for kx in range(1, side // 2):
            tables[parity, kx, :, 0:3] = normal_at(np.full(half, kx), ky, kz, side)
            tables[parity, kx, :, 3:6] = normal_at(np.full(half, -kx), -ky, -kz, side)
            tables[parity, kx, :, 6] = 2.0
        columns = packs[parity]
        order = window_order(parity, (columns[:, 0] == edge) | (columns[:, 1] == edge))
        ky, kz, imag, single = columns[order].T
        angle = 2 * np.pi / side * ((np.outer(ylo, ky) + np.outer(zz, kz)) % side)
        fwd = np.where(imag[None], -np.sin(angle), np.cos(angle))
        share = np.where(single, 1.0, 2.0)
        inv = (fwd * share[None]).T * scale
        forward[parity, 0, :half, :half] = fwd
        forward[parity, 0, half:, half:] = fwd
        inverse[parity, 0, :half, :half] = inv
        inverse[parity, 0, half:, half:] = inv
        for part, kx in ((0, 0), (1, edge)):
            full = np.full(half, kx)
            tables[parity, 0, part, 0:3] = normal_at(full, ky, kz, side)
            tables[parity, 0, part, 3:6] = normal_at(-full, -ky, -kz, side)
            tables[parity, 0, part, 6] = share
    fh, fl = split_table(forward)
    ih, il = split_table(inverse)
    return np.stack([fh, fl]), np.stack([ih, il]), tables.astype(np.float32)


def real_transform(values):
    count = len(values)
    if count == 2:
        return [(values[0] + values[1], None), (values[0] - values[1], None)]
    even = real_transform(values[0::2])
    odd = real_transform(values[1::2])
    half = count // 2
    result = [None] * (half + 1)
    result[0] = (even[0][0] + odd[0][0], None)
    result[half] = (even[0][0] - odd[0][0], None)
    for k in range(1, half // 2):
        (er, ei), (orr, oi) = even[k], odd[k]
        angle = 2 * math.pi * k / count
        c, s = math.cos(angle), math.sin(angle)
        if abs(c - s) < 1e-9:
            tr, ti = (orr + oi) * c, (oi - orr) * c
        else:
            tr, ti = orr * c + oi * s, oi * c - orr * s
        result[k] = (er + tr, ei + ti)
        result[half - k] = (er - tr, ti - ei)
    result[half // 2] = (even[half // 2][0], -odd[half // 2][0])
    return result


def real_inverse(spectrum):
    half = len(spectrum) - 1
    count = 2 * half
    if count == 2:
        return [spectrum[0][0] + spectrum[1][0], spectrum[0][0] - spectrum[1][0]]
    even = [None] * (half // 2 + 1)
    odd = [None] * (half // 2 + 1)
    even[0] = (spectrum[0][0] + spectrum[half][0], None)
    odd[0] = (spectrum[0][0] - spectrum[half][0], None)
    for k in range(1, half // 2):
        (ar, ai), (br, bi) = spectrum[k], spectrum[half - k]
        even[k] = (ar + br, ai - bi)
        dr, di = ar - br, ai + bi
        angle = 2 * math.pi * k / count
        c, s = math.cos(angle), math.sin(angle)
        if abs(c - s) < 1e-9:
            odd[k] = ((dr - di) * c, (dr + di) * c)
        else:
            odd[k] = (dr * c - di * s, dr * s + di * c)
    mid_re, mid_im = spectrum[half // 2]
    even[half // 2] = (mid_re * 2.0, None)
    odd[half // 2] = (mid_im * -2.0, None)
    first, second = real_inverse(even), real_inverse(odd)
    result = []
    for a, b in zip(first, second):
        result += [a, b]
    return result


def potential(entries, normal):
    n0, n1, n2 = normal
    t0 = entries[0] * n0 + entries[5] * n1 + entries[4] * n2
    t1 = entries[5] * n0 + entries[1] * n1 + entries[3] * n2
    t2 = entries[4] * n0 + entries[3] * n1 + entries[2] * n2
    load = (n0 * t0 + n1 * t1 + n2 * t2) * (COUPLING * 1.1)
    return t0 - n0 * load, t1 - n1 * load, t2 - n2 * load


def strain_of(plus, minus, table):
    n0, n1, n2, m0, m1, m2 = table
    u0, u1, u2 = plus
    v0, v1, v2 = minus
    return (
        n0 * u0 + m0 * v0,
        n1 * u1 + m1 * v1,
        n2 * u2 + m2 * v2,
        (n1 * u2 + n2 * u1 + m1 * v2 + m2 * v1) * 0.5,
        (n0 * u2 + n2 * u0 + m0 * v2 + m2 * v0) * 0.5,
        (n0 * u1 + n1 * u0 + m0 * v1 + m1 * v0) * 0.5,
    )


def split_rows(value):
    high = value.astype(BF16)
    return high, (value - high.astype(F32)).astype(BF16)


def product(high, low, table_high, table_low):
    dot = functools.partial(jnp.dot, preferred_element_type=F32)
    return dot(high, table_high) + (dot(low, table_high) + dot(high, table_low))


def column_to_row(column, diagonal):
    return jnp.sum(jnp.where(diagonal, column, 0.0), axis=0, keepdims=True)


def row_to_column(row, diagonal):
    return jnp.sum(jnp.where(diagonal, row, 0.0), axis=1, keepdims=True)


def padded_row(ref):
    row = ref[...].astype(F32)
    return jnp.concatenate([row, jnp.zeros((1, LANES - row.shape[1]), F32)], axis=1)


def slot_choice(owner_ref, place, points, owners, dense):
    lane = lax.broadcasted_iota(jnp.int32, (points, LANES), 1)
    sub = lax.broadcasted_iota(jnp.int32, (points, LANES), 0)
    diagonal = lane == sub
    if not dense:
        return jnp.where(diagonal, 1.0, 0.0), lane
    owner_row = padded_row(owner_ref) - place.astype(F32)
    owner_row = jnp.where(owner_row < 0, owner_row + float(owners), owner_row)
    owner_col = row_to_column(owner_row, diagonal)
    earlier = jnp.where((owner_col == owner_row) & (lane < sub), 1.0, 0.0)
    rank_col = jnp.sum(earlier, axis=1, keepdims=True)
    slot_row = column_to_row(rank_col * owners + owner_col, diagonal)
    return jnp.where((slot_row == sub.astype(F32)) & (lane < points), 1.0, 0.0), lane


def forward_groups(dims, groups, tau, high, low):
    side, slabs = dims

    def step(g, carry):
        at = pl.ds(pl.multiple_of(g * 16, 16), 16)
        for parity in (0, 1):
            values = []
            for x in range(side):
                a, b = tau[2 * x, at], tau[2 * x + 1, at]
                values.append(a + b if parity == 0 else a - b)
            out = real_transform(values)
            for s in range(slabs):
                re, im = out[s] if s else (out[0][0], out[slabs][0])
                for k, v in ((0, re), (1, im)):
                    hi, lo = split_rows(v)
                    high[parity, s, at, k * LANES : (k + 1) * LANES] = hi
                    low[parity, s, at, k * LANES : (k + 1) * LANES] = lo
        return carry

    lax.fori_loop(0, groups, step, 0)


def multiply(high, low, table, spec, done=None):
    slabs, rows, plane = high.shape[1:]
    for parity in (0, 1):
        spec[parity, 0] = product(
            high[parity, 0], low[parity, 0], table[0, parity, 0], table[1, parity, 0]
        )
        spec[parity, 1:] = product(
            high[parity, 1:].reshape((slabs - 1) * rows, plane),
            low[parity, 1:].reshape((slabs - 1) * rows, plane),
            table[0, parity, 1], table[1, parity, 1],
        ).reshape(slabs - 1, rows, plane)
        if done is not None:
            done(parity)


def inverse_rows(spec, at, slabs, emit):
    for yhi in (0, 1):
        parts = []
        for s in range(slabs):
            both = []
            for k in (0, 1):
                lanes = slice(k * LANES, (k + 1) * LANES)
                e, o = spec[0, s, at, lanes], spec[1, s, at, lanes]
                both.append(e + o if yhi == 0 else e - o)
            parts.append(both)
        spectrum = [(parts[0][0], None)] + [tuple(b) for b in parts[1:]]
        spectrum.append((parts[0][1], None))
        for x, v in enumerate(real_inverse(spectrum)):
            emit(2 * x + yhi, v)


def first_kernel(
    dims, place_ref, owner_ref, warm_hbm, moduli_hbm, forward_hbm,
    spec_hbm, both_hbm, mean_ref,
    forward, warm, moduli, spec, tau, high, low, sems,
):
    points, comps, side, owners, dense = dims
    tiles = side**3 // LANES
    parts = 4
    span = side**3 // parts
    stride = moduli.shape[0] // points
    moduli_copies = [
        pltpu.make_async_copy(
            moduli_hbm.at[g], moduli.at[pl.ds(g * stride, 2 * tiles)], sems.at[0]
        )
        for g in range(points)
    ]
    warm_copies = [
        pltpu.make_async_copy(
            warm_hbm.at[:, :, pl.ds(q * span, span)], warm.at[:, :, pl.ds(q * span, span)],
            sems.at[1 + q],
        )
        for q in range(parts)
    ]
    table_copy = pltpu.make_async_copy(forward_hbm, forward, sems.at[1 + parts])
    for copy in moduli_copies + warm_copies + [table_copy]:
        copy.start()
    octets = points // 8
    choose, lane = slot_choice(owner_ref, place_ref[0], points, owners, dense)
    pick = jnp.sum(choose * lane.astype(F32), axis=1, keepdims=True).astype(jnp.int32)
    picks = [jnp.broadcast_to(pick[8 * o : 8 * o + 8], (8, LANES)) for o in range(octets)]
    locals_ = [
        [jnp.clip(picks[o] - 8 * source, 0, 7) for source in range(octets)] for o in range(octets)
    ]
    beyond = [[picks[o] >= 8 * source for source in range(octets)] for o in range(octets)]

    def gather(value):
        if not dense:
            return value
        outs = []
        for o in range(octets):
            best = None
            for source in range(octets):
                got = jnp.take_along_axis(
                    value[8 * source : 8 * source + 8], locals_[o][source], axis=0,
                    mode="promise_in_bounds",
                )
                best = got if best is None else jnp.where(beyond[o][source], got, best)
            outs.append(best)
        return jnp.concatenate(outs, axis=0)

    def load_step(t, sums):
        at = pl.ds(pl.multiple_of(t * LANES, LANES), LANES)
        pair = [
            gather(
                jnp.concatenate(
                    [
                        moduli[pl.ds(8 * o * stride + 2 * t + i, 8, stride=stride), :]
                        for o in range(octets)
                    ],
                    axis=0,
                )
            )
            for i in (0, 1)
        ]
        lamb = pair[0] - REF_MODULUS
        mu = pair[1] * 2.0 - 2.0 * REF_MODULUS
        eps = [gather(warm[c, :, at]) for c in range(comps)]
        extra = lamb * (eps[0] + eps[1] + eps[2])
        for c in range(comps):
            value = mu * eps[c]
            tau[t, c * points : (c + 1) * points] = value + extra if c < 3 else value
        tau[t, comps * points : (comps + 1) * points] = lamb
        tau[t, (comps + 1) * points :] = mu
        return tuple(s + e for s, e in zip(sums, eps + [lamb, mu]))

    zero = jnp.zeros((points, LANES), F32)
    sums = (zero,) * (comps + 2)
    for copy in moduli_copies:
        copy.wait()
    for q in range(parts):
        warm_copies[q].wait()
        sums = lax.fori_loop(q * tiles // parts, (q + 1) * tiles // parts, load_step, sums)
    both_copy = pltpu.make_async_copy(
        tau.at[:, pl.ds(comps * points, 2 * points)], both_hbm, sems.at[0]
    )
    both_copy.start()
    for c in range(comps + 2):
        mean_ref[c * points : (c + 1) * points] = jnp.broadcast_to(
            jnp.sum(sums[c], axis=1, keepdims=True) * (1.0 / side**3), (points, LANES)
        )
    forward_groups((side, side // 2), (comps + 2) * points // 16, tau, high, low)
    table_copy.wait()
    out_copies = []

    def done(parity):
        copy = pltpu.make_async_copy(spec.at[parity], spec_hbm.at[parity], sems.at[1 + parity])
        copy.start()
        out_copies.append(copy)

    multiply(high, low, forward, spec, done)
    both_copy.wait()
    for copy in out_copies:
        copy.wait()


def second_kernel(
    dims,
    part_ref, place_ref, owner_ref, sweeps_ref, weight_ref, conn_ref, grads_ref, table_ref, mean_ref,
    normals_ref, first_hbm, both_hbm, forward_hbm, inverse_hbm,
    *refs,
):
    points, comps, side, devices, node_dev, halo, row_span, nodes_part, owners, dense = dims
    blocks = owners if dense else 1
    leave_refs, (stress_ref, force_ref) = refs[:blocks], refs[blocks : blocks + 2]
    (
        send_ref, first_ref, both, forward, inverse, tau, high, low, spec, pot, edge, full,
        macro_buf, sems, slab_sems, leave_sems,
    ) = refs[blocks + 2 :]
    copies = [
        pltpu.make_async_copy(inverse_hbm, inverse, sems.at[0]),
        pltpu.make_async_copy(both_hbm, both, sems.at[1]),
        pltpu.make_async_copy(forward_hbm, forward, sems.at[2]),
    ]

    def slab_copy(s):
        return pltpu.make_async_copy(
            first_hbm.at[:, pl.ds(s, 1)], first_ref.at[:, pl.ds(s, 1)], slab_sems.at[s]
        )

    for s in range(side // 2):
        slab_copy(s).start()
    for copy in copies:
        copy.start()
    voxels = side**3
    tiles = voxels // LANES
    slabs = side // 2
    part = part_ref[0]
    choose, _ = slot_choice(owner_ref, place_ref[0], points, owners, dense)
    count_col = jnp.sum(choose * padded_row(sweeps_ref), axis=1, keepdims=True)
    weight_row = padded_row(weight_ref)

    exch = table_ref[...]
    dev_sub = lax.broadcasted_iota(jnp.int32, exch.shape, 0)
    below = jnp.sum(jnp.where(dev_sub == (part - 1) * row_span, exch, 0.0), axis=0, keepdims=True)
    above = jnp.sum(jnp.where(dev_sub == (part + 1) * row_span, exch, 0.0), axis=0, keepdims=True)
    parts = devices // row_span
    wide = table_ref.shape[1]
    elane = lax.broadcasted_iota(jnp.int32, (1, wide), 1)
    lane_f = elane.astype(F32)
    part_f = part.astype(F32)
    span = float(nodes_part)
    low_id = jnp.where(part > 0, below + (part_f - 1.0) * span, -1.0)
    high_id = jnp.where(part < parts - 1, above + (part_f + 1.0) * span, -1.0)
    node_row = jnp.where(
        elane < nodes_part,
        part_f * span + lane_f,
        jnp.where(elane < nodes_part + halo, low_id, high_id),
    )
    corner = lax.broadcasted_iota(jnp.int32, (8, LANES), 0)
    corner_lane = lax.broadcasted_iota(jnp.int32, (8, LANES), 1)
    link_rows = conn_ref[...].astype(F32)
    link_rows = jnp.concatenate(
        [link_rows, jnp.zeros((link_rows.shape[0], LANES - 8), F32)], axis=1
    )
    links = jnp.concatenate(
        [row_to_column(link_rows[e : e + 1], corner == corner_lane) for e in range(points // 8)],
        axis=0,
    )
    node_col = jnp.sum(jnp.where(links == lane_f, node_row, 0.0), axis=1, keepdims=True)
    device_col = jnp.floor(node_col * (1.0 / node_dev))
    inner_col = node_col - device_col * node_dev
    nlinks = links.shape[0]
    hit_lane = lax.broadcasted_iota(jnp.int32, (nlinks, devices), 1).astype(F32)
    hit = jnp.where(hit_lane == device_col, 1.0, 0.0)
    flat_lane = lax.broadcasted_iota(jnp.int32, (nlinks, LANES), 1)
    group = flat_lane // node_dev
    inside = jnp.where(
        ((flat_lane - group * node_dev).astype(F32) == inner_col) & (group < 3), 1.0, 0.0
    )
    fetched = jnp.dot(hit, exch[:, :LANES], preferred_element_type=F32,
                      precision=lax.Precision.HIGHEST) * inside
    moved = [
        jnp.sum(jnp.where(group == i, fetched, 0.0), axis=1, keepdims=True) for i in range(3)
    ]
    elements = points // 8
    glane = lax.broadcasted_iota(jnp.int32, (8, LANES), 1)
    spread = []
    for i in range(3):
        acc = jnp.zeros((8, LANES), F32)
        for e in range(elements):
            acc = jnp.where(glane // 8 == e, moved[i][8 * e : 8 * e + 8], acc)
        spread.append(acc)
    grads = [
        jnp.concatenate([grads_ref[j], jnp.zeros((8, LANES - points), F32)], axis=1)
        for j in range(3)
    ]
    grad = [
        [jnp.sum(spread[i] * grads[j], axis=0, keepdims=True) for j in range(3)] for i in range(3)
    ]
    macro_rows = [grad[0][0], grad[1][1], grad[2][2]] + [
        (grad[a][b] + grad[b][a]) * 0.5 for a, b in PAIRS[3:]
    ]
    macro_cols = [jnp.sum(choose * row, axis=1, keepdims=True) for row in macro_rows]


    octets = points // 8
    shift = [
        jnp.broadcast_to(macro_cols[c], (points, LANES)) - mean_ref[c * points : (c + 1) * points]
        for c in range(comps)
    ]
    shift_trace = shift[0] + shift[1] + shift[2]
    macro = [jnp.broadcast_to(col, (points, LANES)) for col in macro_cols]
    again = jnp.broadcast_to(count_col > 1.0, (points, LANES))
    block = send_ref.shape[0] // points

    def send(o, index, value):
        if dense:
            per_owner = points // owners
            send_ref[pl.ds(o * block + index, owners, stride=per_owner * block), :] = value
        else:
            send_ref[pl.ds(8 * o * block + index, 8, stride=block), :] = value

    edge_base = 3 * 4 * slabs
    window_rows = slabs * 2 * WINDOW // LANES
    at_window = lax.broadcasted_iota(jnp.int32, (8, LANES), 1)

    def green_stage(last):
        def load(parity, s, k, o):
            lanes = slice(k * LANES, (k + 1) * LANES)
            if last:
                return [
                    spec[parity, s, c * points + 8 * o : c * points + 8 * o + 8, lanes]
                    for c in range(comps)
                ]
            rows = slice(8 * o, 8 * o + 8)
            raw = [
                first_ref[parity, s, c * points + 8 * o : c * points + 8 * o + 8, lanes]
                for c in range(comps + 2)
            ]
            extra = raw[comps] * shift_trace[rows]
            entries = [raw[c] + raw[comps + 1] * shift[c][rows] for c in range(comps)]
            return [entries[c] + extra if c < 3 else entries[c] for c in range(comps)]

        def step(s, acc):
            acc = list(acc)
            if not last:
                slab_copy(s).wait()
            for k in (0, 1):
                lanes = slice(k * LANES, (k + 1) * LANES)
                results = [[[] for _ in range(comps)] for _ in (0, 1)]
                edges = [[None, None] for _ in range(octets)]
                for parity in (0, 1):
                    table = [
                        jnp.broadcast_to(normals_ref[parity, s, k, d : d + 1, :], (8, LANES))
                        for d in range(7)
                    ]
                    for o in range(octets):
                        rows = slice(8 * o, 8 * o + 8)
                        entries = load(parity, s, k, o)
                        plus = potential(entries, table[0:3])
                        minus = potential(entries, table[3:6])
                        strains = strain_of(plus, minus, table[0:6])
                        for c in range(comps):
                            results[parity][c].append(strains[c])
                        share_l = table[6] * first_ref[
                            parity, s, comps * points + 8 * o : comps * points + 8 * o + 8, lanes
                        ]
                        share_m = table[6] * first_ref[
                            parity, s,
                            (comps + 1) * points + 8 * o : (comps + 1) * points + 8 * o + 8, lanes,
                        ]
                        base = o * (comps + 1)
                        acc[base] = acc[base] + share_l * (strains[0] + strains[1] + strains[2])
                        for c in range(comps):
                            acc[base + 1 + c] = acc[base + 1 + c] + share_m * strains[c]
                        edges[o][parity] = minus
                        for d in range(3):
                            index = (d * 2 + parity) * slabs * 2 + s * 2 + k
                            if last:
                                kept = pot[o, index]
                                send(o, index, jnp.where(again[rows], plus[d], kept))
                            else:
                                pot[o, index] = plus[d]
                if not last:
                    for parity in (0, 1):
                        for c in range(comps):
                            hi, lo = split_rows(jnp.concatenate(results[parity][c], axis=0))
                            high[parity, s, c * points : (c + 1) * points, lanes] = hi
                            low[parity, s, c * points : (c + 1) * points, lanes] = lo
                for o in range(octets):
                    for d in range(3):
                        joined = jnp.where(
                            at_window < SPLIT, edges[o][0][d], edges[o][1][d]
                        )
                        edge[o, d, s * 2 + k] = (
                            jnp.where(again[8 * o : 8 * o + 8], joined, edge[o, d, s * 2 + k])
                            if last else joined
                        )
                        if k == 1:
                            @pl.when(s == 0)
                            def _():
                                for parity in (0, 1):
                                    value = edges[o][parity][d]
                                    if last:
                                        value = jnp.where(
                                            again[8 * o : 8 * o + 8], value, full[o, d, parity]
                                        )
                                    full[o, d, parity] = value
            return tuple(acc)

        zero = jnp.zeros((8, LANES), F32)
        return lax.fori_loop(0, slabs, step, (zero,) * (octets * (comps + 1)))

    first = green_stage(False)
    copies[0].wait()
    multiply(high, low, inverse, spec)

    def field_step(c, carry):
        at = pl.ds(pl.multiple_of(c * points, points), points)
        base = macro_buf[c]

        def emit(tile, value):
            tau[tile, at] = base - value

        inverse_rows(spec, at, slabs, emit)
        return carry

    for c in range(comps):
        macro_buf[c] = macro[c]
    lax.fori_loop(0, comps, field_step, 0)
    copies[1].wait()

    def tau_step(t, carry):
        eps = [tau[t, c * points : (c + 1) * points] for c in range(comps)]
        extra = both[t, :points] * (eps[0] + eps[1] + eps[2])
        mu = both[t, points:]
        for c in range(comps):
            value = mu * eps[c]
            tau[t, c * points : (c + 1) * points] = value + extra if c < 3 else value
        return carry

    lax.fori_loop(0, tiles, tau_step, 0)
    forward_groups((side, slabs), comps * points // 16, tau, high, low)
    copies[2].wait()
    multiply(high, low, forward, spec)
    second = green_stage(True)

    row_lane = lax.broadcasted_iota(jnp.int32, (8, LANES), 1)
    per_row = LANES // WINDOW
    for o in range(octets):
        for d in range(3):
            for v in range(2 * slabs // per_row):
                value = edge[o, d, v * per_row]
                for q in range(1, per_row):
                    moved_q = pltpu.roll(edge[o, d, v * per_row + q], q * WINDOW, 1)
                    value = jnp.where(row_lane >= q * WINDOW, moved_q, value)
                send(o, edge_base + d * (2 * slabs // per_row) + v, value)
            for parity in (0, 1):
                send(o, edge_base + 3 * window_rows + d * 2 + parity, full[o, d, parity])
        value = jnp.zeros((8, LANES), F32)
        for c in range(comps):
            value = jnp.where(row_lane == c, macro[c][8 * o : 8 * o + 8], value)
        send(o, edge_base + 3 * window_rows + 6, value)

    sums = []
    for q in range(comps + 1):
        rows = [
            jnp.where(
                again[8 * o : 8 * o + 8], second[o * (comps + 1) + q], first[o * (comps + 1) + q]
            )
            for o in range(octets)
        ]
        sums.append(
            jnp.sum(jnp.concatenate(rows, axis=0), axis=1, keepdims=True)
            * (1.0 / (2.2 * float(voxels) * float(voxels)))
        )
    lamb_mean = mean_ref[comps * points : (comps + 1) * points]
    mu_mean = mean_ref[(comps + 1) * points :]
    trace = macro[0] + macro[1] + macro[2]
    bulk = (lamb_mean + REF_MODULUS) * trace - sums[0]
    stress_rows = []
    for c in range(comps):
        value = (mu_mean + 2.0 * REF_MODULUS) * macro[c] - sums[1 + c]
        if c < 3:
            value = value + bulk
        stress_rows.append(jnp.sum(choose * value, axis=0, keepdims=True))
    for c in range(comps):
        stress_ref[c : c + 1, :] = stress_rows[c]

    index_of = ((0, 5, 4), (5, 1, 3), (4, 3, 2))
    weighted = [row * weight_row for row in stress_rows]
    loads = jnp.zeros((nlinks, LANES), F32)
    for i in range(3):
        total = sum(grads[j] * weighted[index_of[i][j]] for j in range(3))
        columns = [
            jnp.sum(jnp.where(glane // 8 == e, total, 0.0), axis=1, keepdims=True)
            for e in range(elements)
        ]
        loads = jnp.where(group == i, jnp.concatenate(columns, axis=0), loads)
    loads = loads * inside
    force = lax.dot_general(
        hit, loads, (((0,), (0,)), ((), ())), preferred_element_type=F32,
        precision=lax.Precision.HIGHEST,
    )
    force_ref[...] = force
    last_row = edge_base + 3 * window_rows + 7
    for o in range(octets):
        send(o, last_row, jnp.zeros((8, LANES), F32))
    length = send_ref.shape[0] // blocks
    leave = [
        pltpu.make_async_copy(
            send_ref.at[pl.ds(i * length, length)], leave_refs[i], leave_sems.at[i]
        )
        for i in range(blocks)
    ]
    for copy in leave:
        copy.start()
    for copy in leave:
        copy.wait()


def third_kernel(
    dims, place_ref, *refs
):
    points, comps, side, blocks = dims
    arrived = refs[:blocks]
    normals_ref, inverse_hbm, out_ref, recv_ref, inverse, high, low, spec, sem = refs[blocks:]
    copy = pltpu.make_async_copy(inverse_hbm, inverse, sem)
    copy.start()
    slabs = side // 2
    block = recv_ref.shape[0] // points
    length = arrived[0].shape[0]
    for i in range(blocks):
        source = place_ref[0] - i
        source = jnp.where(source < 0, source + blocks, source) if blocks > 1 else 0
        at = pl.multiple_of(source * length, 8) if blocks > 1 else 0
        recv_ref[pl.ds(at, length)] = arrived[i][...]
    edge_base = 3 * 4 * slabs
    per_row = LANES // WINDOW
    window_rows = 2 * slabs // per_row
    octets = points // 8
    lane = lax.broadcasted_iota(jnp.int32, (8, LANES), 1)

    def fetch(o, index):
        return recv_ref[pl.ds(8 * o * block + index, 8, stride=block), :]

    for s in range(slabs):
        for k in (0, 1):
            window = s * 2 + k
            lanes = slice(k * LANES, (k + 1) * LANES)
            edges = []
            for o in range(octets):
                row = []
                for d in range(3):
                    value = fetch(o, edge_base + d * window_rows + window // per_row)
                    turn = (window % per_row) * WINDOW
                    row.append(pltpu.roll(value, LANES - turn, 1) if turn else value)
                edges.append(row)
            for parity in (0, 1):
                table = [
                    jnp.broadcast_to(normals_ref[parity, s, k, d : d + 1, :], (8, LANES))
                    for d in range(6)
                ]
                if parity == 0:
                    inside = lane < SPLIT
                else:
                    inside = (lane >= SPLIT) & (lane < WINDOW)
                results = [[] for _ in range(comps)]
                for o in range(octets):
                    plus = [
                        fetch(o, (d * 2 + parity) * slabs * 2 + window) for d in range(3)
                    ]
                    if s == 0 and k == 1:
                        minus = [
                            fetch(o, edge_base + 3 * window_rows + d * 2 + parity)
                            for d in range(3)
                        ]
                    else:
                        minus = [jnp.where(inside, edges[o][d], -plus[d]) for d in range(3)]
                    strains = strain_of(plus, minus, table)
                    for c in range(comps):
                        results[c].append(strains[c])
                for c in range(comps):
                    hi, lo = split_rows(jnp.concatenate(results[c], axis=0))
                    high[parity, s, c * points : (c + 1) * points, lanes] = hi
                    low[parity, s, c * points : (c + 1) * points, lanes] = lo
    copy.wait()
    multiply(high, low, inverse, spec)
    tops = [fetch(o, edge_base + 3 * window_rows + 6) for o in range(octets)]
    for c in range(comps):
        base = jnp.concatenate(
            [jnp.broadcast_to(top[:, c : c + 1], (8, LANES)) for top in tops], axis=0
        )

        def emit(tile, value):
            out_ref[c, :, tile * LANES : (tile + 1) * LANES] = base - value

        inverse_rows(spec, slice(c * points, (c + 1) * points), slabs, emit)


def pack_kernel(dims, displacement_ref, halo_ref, out_ref):
    nodes_part, halo = dims
    moved = displacement_ref[...]
    halo_f = halo_ref[...].astype(F32)
    node_dev = moved.shape[1]
    wide = out_ref.shape[1]
    pieces = [moved[0:1], moved[1:2], moved[2:3]]
    pieces.append(jnp.zeros((1, nodes_part - 3 * node_dev), F32))
    pieces += [halo_f[1:2], halo_f[0:1]]
    pieces.append(jnp.zeros((1, wide - nodes_part - 2 * halo), F32))
    out_ref[...] = jnp.broadcast_to(jnp.concatenate(pieces, axis=1), out_ref.shape)


def on_device(
    displacement, shape_grads, point_weights, conn, halo_nodes, warm_strain, moduli, owner, sweeps
):
    axes = ("mesh", "rve")
    points, comps, voxels = warm_strain.shape
    side = round(voxels ** (1.0 / 3.0))
    tiles = voxels // LANES
    slabs = side // 2
    plane = side * side
    owners = lax.axis_size("rve")
    devices = lax.axis_size("mesh") * owners
    node_dev = displacement.shape[1]
    nodes_part = node_dev * owners
    halo = halo_nodes.shape[1]
    per_owner = max(2, points // owners)
    dense = per_owner * owners == points and owners == 8
    wide = -(-(nodes_part + 2 * halo) // LANES) * LANES
    vmem = pl.BlockSpec(memory_space=pltpu.VMEM)
    hbm = pl.BlockSpec(memory_space=pltpu.HBM)
    smem = pl.BlockSpec(memory_space=pltpu.SMEM)
    params = pltpu.CompilerParams(vmem_limit_bytes=62 << 20)

    packed = pl.pallas_call(
        functools.partial(pack_kernel, (nodes_part, halo)),
        out_shape=jax.ShapeDtypeStruct((devices, wide), F32),
        in_specs=[vmem, vmem],
        out_specs=vmem,
        name="pack",
    )(displacement, halo_nodes)
    table = lax.all_to_all(packed, axes, split_axis=0, concat_axis=0, tiled=True)

    owner_row = owner.reshape(1, points)
    sweeps_row = sweeps.reshape(1, points)
    weight_row = point_weights.reshape(1, points)
    part = lax.axis_index("mesh").astype(jnp.int32).reshape(1)
    place = lax.axis_index("rve").astype(jnp.int32).reshape(1)
    warm = warm_strain.transpose(1, 0, 2)
    moduli_rows = (
        moduli.reshape(points, 2, tiles, LANES).transpose(0, 2, 1, 3).reshape(points, -1, LANES)
    )
    forward, inverse, normals = (jnp.asarray(t) for t in build_tables(side))
    rows = comps * points
    more = (comps + 2) * points
    octets = points // 8
    table_scratch = pltpu.VMEM(forward.shape, BF16)
    spec, both, mean = pl.pallas_call(
        functools.partial(first_kernel, (points, comps, side, owners, dense)),
        out_shape=(
            jax.ShapeDtypeStruct((2, slabs, more, plane), F32),
            jax.ShapeDtypeStruct((tiles, 2 * points, LANES), F32),
            jax.ShapeDtypeStruct((more, LANES), F32),
        ),
        in_specs=[smem, vmem, hbm, hbm, hbm],
        out_specs=(hbm, hbm, vmem),
        scratch_shapes=[
            table_scratch,
            pltpu.VMEM((comps, points, voxels), F32),
            pltpu.VMEM((points * (2 * tiles + 8), LANES), F32),
            pltpu.VMEM((2, slabs, more, plane), F32),
            pltpu.VMEM((tiles, more, LANES), F32),
            pltpu.VMEM((2, slabs, more, plane), BF16),
            pltpu.VMEM((2, slabs, more, plane), BF16),
            pltpu.SemaphoreType.DMA((6,)),
        ],
        compiler_params=params,
        cost_estimate=pl.CostEstimate(
            flops=2 * 3 * 16 * more * plane * plane, transcendentals=0, bytes_accessed=4 << 20
        ),
        name="first",
    )(place, owner_row, warm, moduli_rows, forward)

    dims = (points, comps, side, devices, node_dev, halo, owners, nodes_part, owners, dense)
    block = 3 * 4 * slabs + 3 * (2 * slabs * WINDOW // LANES) + 8
    blocks = owners if dense else 1
    *send, stress, force = pl.pallas_call(
        functools.partial(second_kernel, dims),
        out_shape=(
            *(jax.ShapeDtypeStruct((points * block // blocks, LANES), F32),) * blocks,
            jax.ShapeDtypeStruct((8, LANES), F32),
            jax.ShapeDtypeStruct((devices, LANES), F32),
        ),
        in_specs=[smem] * 2 + [vmem] * 8 + [hbm] * 4,
        out_specs=(hbm,) * blocks + (vmem,) * 2,
        scratch_shapes=[
            pltpu.VMEM((points * block, LANES), F32),
            pltpu.VMEM((2, slabs, more, plane), F32),
            pltpu.VMEM((tiles, 2 * points, LANES), F32),
            table_scratch,
            table_scratch,
            pltpu.VMEM((tiles, rows, LANES), F32),
            pltpu.VMEM((2, slabs, rows, plane), BF16),
            pltpu.VMEM((2, slabs, rows, plane), BF16),
            pltpu.VMEM((2, slabs, rows, plane), F32),
            pltpu.VMEM((octets, 3 * 4 * slabs, 8, LANES), F32),
            pltpu.VMEM((octets, 3, 2 * slabs, 8, LANES), F32),
            pltpu.VMEM((octets, 3, 2, 8, LANES), F32),
            pltpu.VMEM((comps, points, LANES), F32),
            pltpu.SemaphoreType.DMA((3,)),
            pltpu.SemaphoreType.DMA((slabs,)),
            pltpu.SemaphoreType.DMA((blocks,)),
        ],
        compiler_params=params,
        cost_estimate=pl.CostEstimate(
            flops=2 * 2 * 3 * 16 * rows * plane * plane, transcendentals=0, bytes_accessed=6 << 20
        ),
        name="second",
    )(
        part, place, owner_row, sweeps_row, weight_row, conn.T, shape_grads, table, mean, normals,
        spec, both, forward, inverse,
    )

    finish = pl.pallas_call(
        functools.partial(third_kernel, (points, comps, side, blocks)),
        out_shape=jax.ShapeDtypeStruct((comps, points, voxels), F32),
        in_specs=[smem] + [vmem] * (blocks + 1) + [hbm],
        out_specs=vmem,
        scratch_shapes=[
            pltpu.VMEM((points * block, LANES), F32),
            table_scratch,
            pltpu.VMEM((2, slabs, rows, plane), BF16),
            pltpu.VMEM((2, slabs, rows, plane), BF16),
            pltpu.VMEM((2, slabs, rows, plane), F32),
            pltpu.SemaphoreType.DMA,
        ],
        compiler_params=pltpu.CompilerParams(vmem_limit_bytes=24 << 20),
        cost_estimate=pl.CostEstimate(
            flops=2 * 3 * 16 * rows * plane * plane, transcendentals=0, bytes_accessed=4 << 20
        ),
        name="third",
    )
    comps_out = stress[:comps, :points]
    if dense:
        arrived = [send[0]] + [
            lax.ppermute(send[i], "rve", [(j, (j + i) % owners) for j in range(owners)])
            for i in range(1, owners)
        ]
        micro = finish(place, *arrived, normals, inverse).transpose(1, 0, 2)
    else:
        slots = owners * per_owner
        final = finish(place, send[0], normals, inverse).transpose(1, 0, 2)
        order = jnp.arange(points, dtype=jnp.int32)
        same = owner[:, None] == owner[None, :]
        rank = jnp.sum((same & (order[None, :] < order[:, None])).astype(jnp.int32), axis=1)
        slot = owner * per_owner + rank
        fields = jnp.zeros((slots, comps, voxels), F32).at[slot].set(final)
        flags = jnp.zeros((slots,), F32).at[slot].set(1.0)
        fields = lax.all_to_all(fields, "rve", split_axis=0, concat_axis=0, tiled=True)
        flags = lax.all_to_all(flags, "rve", split_axis=0, concat_axis=0, tiled=True)
        filled = jnp.nonzero(flags > 0.5, size=points)[0].astype(jnp.int32)
        micro = fields[filled]
    pieces = lax.all_to_all(force, axes, split_axis=0, concat_axis=0, tiled=True)
    nodal = jnp.sum(pieces, axis=0)[: 3 * node_dev].reshape(3, node_dev)
    return (nodal, comps_out, micro)


def solution(mesh):
    both = ("mesh", "rve")
    in_specs = (
        P(None, both), P(None, None, both), P(both), P(None, both), P(None, "mesh"),
        P(both, None, None), P(both, None, None), P(both), P(both),
    )
    out_specs = (P(None, both), P(None, both), P(both, None, None))

    return jax.shard_map(
        on_device, mesh=mesh, in_specs=in_specs, out_specs=out_specs, check_vma=False
    )
```

```python
import functools
import math

import jax
import jax.numpy as jnp
import numpy as np
from jax import lax
from jax.experimental import pallas as pl
from jax.experimental.pallas import tpu as pltpu
from jax.sharding import PartitionSpec as P


REF_MODULUS = 1.1
COUPLING = 2.2 / (1.1 * 3.3)
PAIRS = ((0, 0), (1, 1), (2, 2), (1, 2), (0, 2), (0, 1))
F32 = jnp.float32
BF16 = jnp.bfloat16
LANES = 128
WINDOW = 32
SPLIT = 24


def signed_waves(side):
    wave = np.arange(side)
    return np.where(wave < side // 2, wave, wave - side)


def normal_at(kx, ky, kz, side):
    signed = signed_waves(side)
    xi = np.stack([signed[kx % side], signed[ky % side], signed[kz % side]]).astype(np.float64)
    length = np.sqrt((xi * xi).sum(0))
    return np.where(length > 0, xi / np.where(length > 0, length, 1.0), 0.0)


def plane_sets(side):
    packs = []
    for parity in (0, 1):
        columns, seen = [], set()
        for ky in range(parity, side, 2):
            for kz in range(side):
                if (ky, kz) in seen:
                    continue
                mirror = (-ky % side, -kz % side)
                seen.update({(ky, kz), mirror})
                if mirror == (ky, kz):
                    columns.append((ky, kz, 0, 1))
                else:
                    columns += [(ky, kz, 0, 0), (ky, kz, 1, 0)]
        packs.append(np.array(columns))
    return packs


def window_order(parity, at_edge):
    edge, rest = list(np.flatnonzero(at_edge)), list(np.flatnonzero(~at_edge))
    lead = SPLIT if parity else 0
    limit = WINDOW - SPLIT if parity else SPLIT
    assert len(edge) <= limit
    return np.array(rest[:lead] + edge + rest[lead:])


def split_table(table):
    high = np.asarray(table, np.float32).astype(jnp.bfloat16)
    low = (np.asarray(table, np.float64) - high.astype(np.float64)).astype(jnp.bfloat16)
    return high, low


def build_tables(side):
    plane = side * side
    half = plane // 2
    edge = side // 2
    ylo, zz = np.divmod(np.arange(half), side)
    scale = 1.0 / (2.2 * side**3)
    forward = np.zeros((2, 2, plane, plane))
    inverse = np.zeros((2, 2, plane, plane))
    tables = np.zeros((2, side // 2, 2, 8, half))
    packs = plane_sets(side)
    for parity in (0, 1):
        kyi, kz = np.divmod(np.arange(half), side)
        ky = 2 * kyi + parity
        order = window_order(parity, (ky == edge) | (kz == edge))
        ky, kz = ky[order], kz[order]
        angle = 2 * np.pi / side * ((np.outer(ylo, ky) + np.outer(zz, kz)) % side)
        c, s = np.cos(angle), np.sin(angle)
        forward[parity, 1] = np.block([[c, -s], [s, c]])
        inverse[parity, 1] = np.block([[c.T, s.T], [-s.T, c.T]]) * scale
        for kx in range(1, side // 2):
            tables[parity, kx, :, 0:3] = normal_at(np.full(half, kx), ky, kz, side)
            tables[parity, kx, :, 3:6] = normal_at(np.full(half, -kx), -ky, -kz, side)
            tables[parity, kx, :, 6] = 2.0
        columns = packs[parity]
        order = window_order(parity, (columns[:, 0] == edge) | (columns[:, 1] == edge))
        ky, kz, imag, single = columns[order].T
        angle = 2 * np.pi / side * ((np.outer(ylo, ky) + np.outer(zz, kz)) % side)
        fwd = np.where(imag[None], -np.sin(angle), np.cos(angle))
        share = np.where(single, 1.0, 2.0)
        inv = (fwd * share[None]).T * scale
        forward[parity, 0, :half, :half] = fwd
        forward[parity, 0, half:, half:] = fwd
        inverse[parity, 0, :half, :half] = inv
        inverse[parity, 0, half:, half:] = inv
        for part, kx in ((0, 0), (1, edge)):
            full = np.full(half, kx)
            tables[parity, 0, part, 0:3] = normal_at(full, ky, kz, side)
            tables[parity, 0, part, 3:6] = normal_at(-full, -ky, -kz, side)
            tables[parity, 0, part, 6] = share
    fh, fl = split_table(forward)
    ih, il = split_table(inverse)
    return np.stack([fh, fl]), np.stack([ih, il]), tables.astype(np.float32)


def real_transform(values):
    count = len(values)
    if count == 2:
        return [(values[0] + values[1], None), (values[0] - values[1], None)]
    even = real_transform(values[0::2])
    odd = real_transform(values[1::2])
    half = count // 2
    result = [None] * (half + 1)
    result[0] = (even[0][0] + odd[0][0], None)
    result[half] = (even[0][0] - odd[0][0], None)
    for k in range(1, half // 2):
        (er, ei), (orr, oi) = even[k], odd[k]
        angle = 2 * math.pi * k / count
        c, s = math.cos(angle), math.sin(angle)
        if abs(c - s) < 1e-9:
            tr, ti = (orr + oi) * c, (oi - orr) * c
        else:
            tr, ti = orr * c + oi * s, oi * c - orr * s
        result[k] = (er + tr, ei + ti)
        result[half - k] = (er - tr, ti - ei)
    result[half // 2] = (even[half // 2][0], -odd[half // 2][0])
    return result


def real_inverse(spectrum):
    half = len(spectrum) - 1
    count = 2 * half
    if count == 2:
        return [spectrum[0][0] + spectrum[1][0], spectrum[0][0] - spectrum[1][0]]
    even = [None] * (half // 2 + 1)
    odd = [None] * (half // 2 + 1)
    even[0] = (spectrum[0][0] + spectrum[half][0], None)
    odd[0] = (spectrum[0][0] - spectrum[half][0], None)
    for k in range(1, half // 2):
        (ar, ai), (br, bi) = spectrum[k], spectrum[half - k]
        even[k] = (ar + br, ai - bi)
        dr, di = ar - br, ai + bi
        angle = 2 * math.pi * k / count
        c, s = math.cos(angle), math.sin(angle)
        if abs(c - s) < 1e-9:
            odd[k] = ((dr - di) * c, (dr + di) * c)
        else:
            odd[k] = (dr * c - di * s, dr * s + di * c)
    mid_re, mid_im = spectrum[half // 2]
    even[half // 2] = (mid_re * 2.0, None)
    odd[half // 2] = (mid_im * -2.0, None)
    first, second = real_inverse(even), real_inverse(odd)
    result = []
    for a, b in zip(first, second):
        result += [a, b]
    return result


def potential(entries, normal):
    n0, n1, n2 = normal
    t0 = entries[0] * n0 + entries[5] * n1 + entries[4] * n2
    t1 = entries[5] * n0 + entries[1] * n1 + entries[3] * n2
    t2 = entries[4] * n0 + entries[3] * n1 + entries[2] * n2
    load = (n0 * t0 + n1 * t1 + n2 * t2) * (COUPLING * 1.1)
    return t0 - n0 * load, t1 - n1 * load, t2 - n2 * load


def strain_of(plus, minus, table):
    n0, n1, n2, m0, m1, m2 = table
    u0, u1, u2 = plus
    v0, v1, v2 = minus
    return (
        n0 * u0 + m0 * v0,
        n1 * u1 + m1 * v1,
        n2 * u2 + m2 * v2,
        (n1 * u2 + n2 * u1 + m1 * v2 + m2 * v1) * 0.5,
        (n0 * u2 + n2 * u0 + m0 * v2 + m2 * v0) * 0.5,
        (n0 * u1 + n1 * u0 + m0 * v1 + m1 * v0) * 0.5,
    )


def split_rows(value):
    high = value.astype(BF16)
    return high, (value - high.astype(F32)).astype(BF16)


def product(high, low, table_high, table_low):
    dot = functools.partial(jnp.dot, preferred_element_type=F32)
    return dot(high, table_high) + (dot(low, table_high) + dot(high, table_low))


def column_to_row(column, diagonal):
    return jnp.sum(jnp.where(diagonal, column, 0.0), axis=0, keepdims=True)


def row_to_column(row, diagonal):
    return jnp.sum(jnp.where(diagonal, row, 0.0), axis=1, keepdims=True)


def padded_row(ref):
    row = ref[...].astype(F32)
    return jnp.concatenate([row, jnp.zeros((1, LANES - row.shape[1]), F32)], axis=1)


def slot_choice(owner_ref, place, points, owners, dense):
    lane = lax.broadcasted_iota(jnp.int32, (points, LANES), 1)
    sub = lax.broadcasted_iota(jnp.int32, (points, LANES), 0)
    diagonal = lane == sub
    if not dense:
        return jnp.where(diagonal, 1.0, 0.0), lane
    owner_row = padded_row(owner_ref) - place.astype(F32)
    owner_row = jnp.where(owner_row < 0, owner_row + float(owners), owner_row)
    owner_col = row_to_column(owner_row, diagonal)
    earlier = jnp.where((owner_col == owner_row) & (lane < sub), 1.0, 0.0)
    rank_col = jnp.sum(earlier, axis=1, keepdims=True)
    slot_row = column_to_row(rank_col * owners + owner_col, diagonal)
    return jnp.where((slot_row == sub.astype(F32)) & (lane < points), 1.0, 0.0), lane


def forward_groups(dims, groups, tau, high, low):
    side, slabs = dims

    def step(g, carry):
        at = pl.ds(pl.multiple_of(g * 16, 16), 16)
        for parity in (0, 1):
            values = []
            for x in range(side):
                a, b = tau[2 * x, at], tau[2 * x + 1, at]
                values.append(a + b if parity == 0 else a - b)
            out = real_transform(values)
            for s in range(slabs):
                re, im = out[s] if s else (out[0][0], out[slabs][0])
                for k, v in ((0, re), (1, im)):
                    hi, lo = split_rows(v)
                    high[parity, s, at, k * LANES : (k + 1) * LANES] = hi
                    low[parity, s, at, k * LANES : (k + 1) * LANES] = lo
        return carry

    lax.fori_loop(0, groups, step, 0)


def multiply(high, low, table, spec, done=None):
    slabs, rows, plane = high.shape[1:]
    for parity in (0, 1):
        spec[parity, 0] = product(
            high[parity, 0], low[parity, 0], table[0, parity, 0], table[1, parity, 0]
        )
        spec[parity, 1:] = product(
            high[parity, 1:].reshape((slabs - 1) * rows, plane),
            low[parity, 1:].reshape((slabs - 1) * rows, plane),
            table[0, parity, 1], table[1, parity, 1],
        ).reshape(slabs - 1, rows, plane)
        if done is not None:
            done(parity)


def inverse_rows(spec, at, slabs, emit):
    for yhi in (0, 1):
        parts = []
        for s in range(slabs):
            both = []
            for k in (0, 1):
                lanes = slice(k * LANES, (k + 1) * LANES)
                e, o = spec[0, s, at, lanes], spec[1, s, at, lanes]
                both.append(e + o if yhi == 0 else e - o)
            parts.append(both)
        spectrum = [(parts[0][0], None)] + [tuple(b) for b in parts[1:]]
        spectrum.append((parts[0][1], None))
        for x, v in enumerate(real_inverse(spectrum)):
            emit(2 * x + yhi, v)


def first_kernel(
    dims, place_ref, owner_ref, warm_hbm, moduli_hbm, forward_hbm,
    spec_hbm, both_hbm, mean_ref,
    forward, warm, moduli, spec, tau, high, low, sems,
):
    points, comps, side, owners, dense = dims
    tiles = side**3 // LANES
    parts = 4
    span = side**3 // parts
    stride = moduli.shape[0] // points
    moduli_copies = [
        pltpu.make_async_copy(
            moduli_hbm.at[g], moduli.at[pl.ds(g * stride, 2 * tiles)], sems.at[0]
        )
        for g in range(points)
    ]
    warm_copies = [
        pltpu.make_async_copy(
            warm_hbm.at[:, :, pl.ds(q * span, span)], warm.at[:, :, pl.ds(q * span, span)],
            sems.at[1 + q],
        )
        for q in range(parts)
    ]
    table_copy = pltpu.make_async_copy(forward_hbm, forward, sems.at[1 + parts])
    for copy in moduli_copies + warm_copies + [table_copy]:
        copy.start()
    octets = points // 8
    choose, lane = slot_choice(owner_ref, place_ref[0], points, owners, dense)
    pick = jnp.sum(choose * lane.astype(F32), axis=1, keepdims=True).astype(jnp.int32)
    picks = [jnp.broadcast_to(pick[8 * o : 8 * o + 8], (8, LANES)) for o in range(octets)]
    locals_ = [
        [jnp.clip(picks[o] - 8 * source, 0, 7) for source in range(octets)] for o in range(octets)
    ]
    beyond = [[picks[o] >= 8 * source for source in range(octets)] for o in range(octets)]

    def gather(value):
        if not dense:
            return value
        outs = []
        for o in range(octets):
            best = None
            for source in range(octets):
                got = jnp.take_along_axis(
                    value[8 * source : 8 * source + 8], locals_[o][source], axis=0,
                    mode="promise_in_bounds",
                )
                best = got if best is None else jnp.where(beyond[o][source], got, best)
            outs.append(best)
        return jnp.concatenate(outs, axis=0)

    def load_step(t, sums):
        at = pl.ds(pl.multiple_of(t * LANES, LANES), LANES)
        pair = [
            gather(
                jnp.concatenate(
                    [
                        moduli[pl.ds(8 * o * stride + 2 * t + i, 8, stride=stride), :]
                        for o in range(octets)
                    ],
                    axis=0,
                )
            )
            for i in (0, 1)
        ]
        lamb = pair[0] - REF_MODULUS
        mu = pair[1] * 2.0 - 2.0 * REF_MODULUS
        eps = [gather(warm[c, :, at]) for c in range(comps)]
        extra = lamb * (eps[0] + eps[1] + eps[2])
        for c in range(comps):
            value = mu * eps[c]
            tau[t, c * points : (c + 1) * points] = value + extra if c < 3 else value
        tau[t, comps * points : (comps + 1) * points] = lamb
        tau[t, (comps + 1) * points :] = mu
        return tuple(s + e for s, e in zip(sums, eps + [lamb, mu]))

    zero = jnp.zeros((points, LANES), F32)
    sums = (zero,) * (comps + 2)
    for copy in moduli_copies:
        copy.wait()
    for q in range(parts):
        warm_copies[q].wait()
        sums = lax.fori_loop(q * tiles // parts, (q + 1) * tiles // parts, load_step, sums)
    both_copy = pltpu.make_async_copy(
        tau.at[:, pl.ds(comps * points, 2 * points)], both_hbm, sems.at[0]
    )
    both_copy.start()
    for c in range(comps + 2):
        mean_ref[c * points : (c + 1) * points] = jnp.broadcast_to(
            jnp.sum(sums[c], axis=1, keepdims=True) * (1.0 / side**3), (points, LANES)
        )
    forward_groups((side, side // 2), (comps + 2) * points // 16, tau, high, low)
    table_copy.wait()
    out_copies = []

    def done(parity):
        copy = pltpu.make_async_copy(spec.at[parity], spec_hbm.at[parity], sems.at[1 + parity])
        copy.start()
        out_copies.append(copy)

    multiply(high, low, forward, spec, done)
    both_copy.wait()
    for copy in out_copies:
        copy.wait()


def second_kernel(
    dims,
    part_ref, place_ref, owner_ref, sweeps_ref, weight_ref, conn_ref, grads_ref, table_ref, mean_ref,
    normals_ref, first_hbm, both_hbm, forward_hbm, inverse_hbm,
    *refs,
):
    points, comps, side, devices, node_dev, halo, row_span, nodes_part, owners, dense = dims
    blocks = owners if dense else 1
    leave_refs, (stress_ref, force_ref) = refs[:blocks], refs[blocks : blocks + 2]
    (
        send_ref, first_ref, both, forward, inverse, tau, high, low, spec, pot, edge, full,
        macro_buf, sems, slab_sems,
    ) = refs[blocks + 2 :]
    copies = [
        pltpu.make_async_copy(inverse_hbm, inverse, sems.at[0]),
        pltpu.make_async_copy(both_hbm, both, sems.at[1]),
        pltpu.make_async_copy(forward_hbm, forward, sems.at[2]),
    ]

    def slab_copy(s):
        return pltpu.make_async_copy(
            first_hbm.at[:, pl.ds(s, 1)], first_ref.at[:, pl.ds(s, 1)], slab_sems.at[s]
        )

    for s in range(side // 2):
        slab_copy(s).start()
    voxels = side**3
    tiles = voxels // LANES
    slabs = side // 2
    part = part_ref[0]
    choose, _ = slot_choice(owner_ref, place_ref[0], points, owners, dense)
    count_col = jnp.sum(choose * padded_row(sweeps_ref), axis=1, keepdims=True)
    weight_row = padded_row(weight_ref)

    exch = table_ref[...]
    dev_sub = lax.broadcasted_iota(jnp.int32, exch.shape, 0)
    below = jnp.sum(jnp.where(dev_sub == (part - 1) * row_span, exch, 0.0), axis=0, keepdims=True)
    above = jnp.sum(jnp.where(dev_sub == (part + 1) * row_span, exch, 0.0), axis=0, keepdims=True)
    parts = devices // row_span
    wide = table_ref.shape[1]
    elane = lax.broadcasted_iota(jnp.int32, (1, wide), 1)
    lane_f = elane.astype(F32)
    part_f = part.astype(F32)
    span = float(nodes_part)
    low_id = jnp.where(part > 0, below + (part_f - 1.0) * span, -1.0)
    high_id = jnp.where(part < parts - 1, above + (part_f + 1.0) * span, -1.0)
    node_row = jnp.where(
        elane < nodes_part,
        part_f * span + lane_f,
        jnp.where(elane < nodes_part + halo, low_id, high_id),
    )
    corner = lax.broadcasted_iota(jnp.int32, (8, LANES), 0)
    corner_lane = lax.broadcasted_iota(jnp.int32, (8, LANES), 1)
    link_rows = conn_ref[...].astype(F32)
    link_rows = jnp.concatenate(
        [link_rows, jnp.zeros((link_rows.shape[0], LANES - 8), F32)], axis=1
    )
    links = jnp.concatenate(
        [row_to_column(link_rows[e : e + 1], corner == corner_lane) for e in range(points // 8)],
        axis=0,
    )
    node_col = jnp.sum(jnp.where(links == lane_f, node_row, 0.0), axis=1, keepdims=True)
    device_col = jnp.floor(node_col * (1.0 / node_dev))
    inner_col = node_col - device_col * node_dev
    nlinks = links.shape[0]
    hit_lane = lax.broadcasted_iota(jnp.int32, (nlinks, devices), 1).astype(F32)
    hit = jnp.where(hit_lane == device_col, 1.0, 0.0)
    flat_lane = lax.broadcasted_iota(jnp.int32, (nlinks, LANES), 1)
    group = flat_lane // node_dev
    inside = jnp.where(
        ((flat_lane - group * node_dev).astype(F32) == inner_col) & (group < 3), 1.0, 0.0
    )
    fetched = jnp.dot(hit, exch[:, :LANES], preferred_element_type=F32,
                      precision=lax.Precision.HIGHEST) * inside
    moved = [
        jnp.sum(jnp.where(group == i, fetched, 0.0), axis=1, keepdims=True) for i in range(3)
    ]
    elements = points // 8
    glane = lax.broadcasted_iota(jnp.int32, (8, LANES), 1)
    spread = []
    for i in range(3):
        acc = jnp.zeros((8, LANES), F32)
        for e in range(elements):
            acc = jnp.where(glane // 8 == e, moved[i][8 * e : 8 * e + 8], acc)
        spread.append(acc)
    grads = [
        jnp.concatenate([grads_ref[j], jnp.zeros((8, LANES - points), F32)], axis=1)
        for j in range(3)
    ]
    grad = [
        [jnp.sum(spread[i] * grads[j], axis=0, keepdims=True) for j in range(3)] for i in range(3)
    ]
    macro_rows = [grad[0][0], grad[1][1], grad[2][2]] + [
        (grad[a][b] + grad[b][a]) * 0.5 for a, b in PAIRS[3:]
    ]
    macro_cols = [jnp.sum(choose * row, axis=1, keepdims=True) for row in macro_rows]


    octets = points // 8
    shift = [
        jnp.broadcast_to(macro_cols[c], (points, LANES)) - mean_ref[c * points : (c + 1) * points]
        for c in range(comps)
    ]
    shift_trace = shift[0] + shift[1] + shift[2]
    macro = [jnp.broadcast_to(col, (points, LANES)) for col in macro_cols]
    again = jnp.broadcast_to(count_col > 1.0, (points, LANES))
    block = send_ref.shape[0] // points

    def send(o, index, value):
        if dense:
            per_owner = points // owners
            send_ref[pl.ds(o * block + index, owners, stride=per_owner * block), :] = value
        else:
            send_ref[pl.ds(8 * o * block + index, 8, stride=block), :] = value

    edge_base = 3 * 4 * slabs
    window_rows = slabs * 2 * WINDOW // LANES
    at_window = lax.broadcasted_iota(jnp.int32, (8, LANES), 1)

    def green_stage(last):
        def load(parity, s, k, o):
            lanes = slice(k * LANES, (k + 1) * LANES)
            if last:
                return [
                    spec[parity, s, c * points + 8 * o : c * points + 8 * o + 8, lanes]
                    for c in range(comps)
                ]
            rows = slice(8 * o, 8 * o + 8)
            raw = [
                first_ref[parity, s, c * points + 8 * o : c * points + 8 * o + 8, lanes]
                for c in range(comps + 2)
            ]
            extra = raw[comps] * shift_trace[rows]
            entries = [raw[c] + raw[comps + 1] * shift[c][rows] for c in range(comps)]
            return [entries[c] + extra if c < 3 else entries[c] for c in range(comps)]

        def step(s, acc):
            acc = list(acc)
            if not last:
                slab_copy(s).wait()
            for k in (0, 1):
                lanes = slice(k * LANES, (k + 1) * LANES)
                results = [[[] for _ in range(comps)] for _ in (0, 1)]
                edges = [[None, None] for _ in range(octets)]
                for parity in (0, 1):
                    table = [
                        jnp.broadcast_to(normals_ref[parity, s, k, d : d + 1, :], (8, LANES))
                        for d in range(7)
                    ]
                    for o in range(octets):
                        rows = slice(8 * o, 8 * o + 8)
                        entries = load(parity, s, k, o)
                        plus = potential(entries, table[0:3])
                        minus = potential(entries, table[3:6])
                        strains = strain_of(plus, minus, table[0:6])
                        for c in range(comps):
                            results[parity][c].append(strains[c])
                        share_l = table[6] * first_ref[
                            parity, s, comps * points + 8 * o : comps * points + 8 * o + 8, lanes
                        ]
                        share_m = table[6] * first_ref[
                            parity, s,
                            (comps + 1) * points + 8 * o : (comps + 1) * points + 8 * o + 8, lanes,
                        ]
                        base = o * (comps + 1)
                        acc[base] = acc[base] + share_l * (strains[0] + strains[1] + strains[2])
                        for c in range(comps):
                            acc[base + 1 + c] = acc[base + 1 + c] + share_m * strains[c]
                        edges[o][parity] = minus
                        for d in range(3):
                            index = (d * 2 + parity) * slabs * 2 + s * 2 + k
                            if last:
                                kept = pot[o, index]
                                send(o, index, jnp.where(again[rows], plus[d], kept))
                            else:
                                pot[o, index] = plus[d]
                if not last:
                    for parity in (0, 1):
                        for c in range(comps):
                            hi, lo = split_rows(jnp.concatenate(results[parity][c], axis=0))
                            high[parity, s, c * points : (c + 1) * points, lanes] = hi
                            low[parity, s, c * points : (c + 1) * points, lanes] = lo
                for o in range(octets):
                    for d in range(3):
                        joined = jnp.where(
                            at_window < SPLIT, edges[o][0][d], edges[o][1][d]
                        )
                        edge[o, d, s * 2 + k] = (
                            jnp.where(again[8 * o : 8 * o + 8], joined, edge[o, d, s * 2 + k])
                            if last else joined
                        )
                        if k == 1:
                            @pl.when(s == 0)
                            def _():
                                for parity in (0, 1):
                                    value = edges[o][parity][d]
                                    if last:
                                        value = jnp.where(
                                            again[8 * o : 8 * o + 8], value, full[o, d, parity]
                                        )
                                    full[o, d, parity] = value
            return tuple(acc)

        zero = jnp.zeros((8, LANES), F32)
        return lax.fori_loop(0, slabs, step, (zero,) * (octets * (comps + 1)))

    copies[0].start()
    first = green_stage(False)
    for copy in copies[1:]:
        copy.start()
    copies[0].wait()
    multiply(high, low, inverse, spec)

    def field_step(c, carry):
        at = pl.ds(pl.multiple_of(c * points, points), points)
        base = macro_buf[c]

        def emit(tile, value):
            tau[tile, at] = base - value

        inverse_rows(spec, at, slabs, emit)
        return carry

    for c in range(comps):
        macro_buf[c] = macro[c]
    lax.fori_loop(0, comps, field_step, 0)
    copies[1].wait()

    def tau_step(t, carry):
        eps = [tau[t, c * points : (c + 1) * points] for c in range(comps)]
        extra = both[t, :points] * (eps[0] + eps[1] + eps[2])
        mu = both[t, points:]
        for c in range(comps):
            value = mu * eps[c]
            tau[t, c * points : (c + 1) * points] = value + extra if c < 3 else value
        return carry

    lax.fori_loop(0, tiles, tau_step, 0)
    forward_groups((side, slabs), comps * points // 16, tau, high, low)
    copies[2].wait()
    multiply(high, low, forward, spec)
    second = green_stage(True)

    row_lane = lax.broadcasted_iota(jnp.int32, (8, LANES), 1)
    per_row = LANES // WINDOW
    for o in range(octets):
        for d in range(3):
            for v in range(2 * slabs // per_row):
                value = edge[o, d, v * per_row]
                for q in range(1, per_row):
                    moved_q = pltpu.roll(edge[o, d, v * per_row + q], q * WINDOW, 1)
                    value = jnp.where(row_lane >= q * WINDOW, moved_q, value)
                send(o, edge_base + d * (2 * slabs // per_row) + v, value)
            for parity in (0, 1):
                send(o, edge_base + 3 * window_rows + d * 2 + parity, full[o, d, parity])
        value = jnp.zeros((8, LANES), F32)
        for c in range(comps):
            value = jnp.where(row_lane == c, macro[c][8 * o : 8 * o + 8], value)
        send(o, edge_base + 3 * window_rows + 6, value)
        send(o, edge_base + 3 * window_rows + 7, jnp.zeros((8, LANES), F32))
    length = send_ref.shape[0] // blocks
    for i in range(blocks):
        leave_refs[i][...] = send_ref[i * length : (i + 1) * length]

    sums = []
    for q in range(comps + 1):
        rows = [
            jnp.where(
                again[8 * o : 8 * o + 8], second[o * (comps + 1) + q], first[o * (comps + 1) + q]
            )
            for o in range(octets)
        ]
        sums.append(
            jnp.sum(jnp.concatenate(rows, axis=0), axis=1, keepdims=True)
            * (1.0 / (2.2 * float(voxels) * float(voxels)))
        )
    lamb_mean = mean_ref[comps * points : (comps + 1) * points]
    mu_mean = mean_ref[(comps + 1) * points :]
    trace = macro[0] + macro[1] + macro[2]
    bulk = (lamb_mean + REF_MODULUS) * trace - sums[0]
    stress_rows = []
    for c in range(comps):
        value = (mu_mean + 2.0 * REF_MODULUS) * macro[c] - sums[1 + c]
        if c < 3:
            value = value + bulk
        stress_rows.append(jnp.sum(choose * value, axis=0, keepdims=True))
    for c in range(comps):
        stress_ref[c : c + 1, :] = stress_rows[c]

    index_of = ((0, 5, 4), (5, 1, 3), (4, 3, 2))
    weighted = [row * weight_row for row in stress_rows]
    loads = jnp.zeros((nlinks, LANES), F32)
    for i in range(3):
        total = sum(grads[j] * weighted[index_of[i][j]] for j in range(3))
        columns = [
            jnp.sum(jnp.where(glane // 8 == e, total, 0.0), axis=1, keepdims=True)
            for e in range(elements)
        ]
        loads = jnp.where(group == i, jnp.concatenate(columns, axis=0), loads)
    loads = loads * inside
    force = lax.dot_general(
        hit, loads, (((0,), (0,)), ((), ())), preferred_element_type=F32,
        precision=lax.Precision.HIGHEST,
    )
    force_ref[...] = force


def third_kernel(
    dims, place_ref, *refs
):
    points, comps, side, blocks = dims
    arrived = refs[:blocks]
    normals_ref, inverse_hbm, out_ref, recv_ref, inverse, high, low, spec, sem = refs[blocks:]
    copy = pltpu.make_async_copy(inverse_hbm, inverse, sem)
    copy.start()
    slabs = side // 2
    block = recv_ref.shape[0] // points
    length = arrived[0].shape[0]
    for i in range(blocks):
        source = place_ref[0] - i
        source = jnp.where(source < 0, source + blocks, source) if blocks > 1 else 0
        at = pl.multiple_of(source * length, 8) if blocks > 1 else 0
        recv_ref[pl.ds(at, length)] = arrived[i][...]
    edge_base = 3 * 4 * slabs
    per_row = LANES // WINDOW
    window_rows = 2 * slabs // per_row
    octets = points // 8
    lane = lax.broadcasted_iota(jnp.int32, (8, LANES), 1)

    def fetch(o, index):
        return recv_ref[pl.ds(8 * o * block + index, 8, stride=block), :]

    for s in range(slabs):
        for k in (0, 1):
            window = s * 2 + k
            lanes = slice(k * LANES, (k + 1) * LANES)
            edges = []
            for o in range(octets):
                row = []
                for d in range(3):
                    value = fetch(o, edge_base + d * window_rows + window // per_row)
                    turn = (window % per_row) * WINDOW
                    row.append(pltpu.roll(value, LANES - turn, 1) if turn else value)
                edges.append(row)
            for parity in (0, 1):
                table = [
                    jnp.broadcast_to(normals_ref[parity, s, k, d : d + 1, :], (8, LANES))
                    for d in range(6)
                ]
                if parity == 0:
                    inside = lane < SPLIT
                else:
                    inside = (lane >= SPLIT) & (lane < WINDOW)
                results = [[] for _ in range(comps)]
                for o in range(octets):
                    plus = [
                        fetch(o, (d * 2 + parity) * slabs * 2 + window) for d in range(3)
                    ]
                    if s == 0 and k == 1:
                        minus = [
                            fetch(o, edge_base + 3 * window_rows + d * 2 + parity)
                            for d in range(3)
                        ]
                    else:
                        minus = [jnp.where(inside, edges[o][d], -plus[d]) for d in range(3)]
                    strains = strain_of(plus, minus, table)
                    for c in range(comps):
                        results[c].append(strains[c])
                for c in range(comps):
                    hi, lo = split_rows(jnp.concatenate(results[c], axis=0))
                    high[parity, s, c * points : (c + 1) * points, lanes] = hi
                    low[parity, s, c * points : (c + 1) * points, lanes] = lo
    copy.wait()
    multiply(high, low, inverse, spec)
    tops = [fetch(o, edge_base + 3 * window_rows + 6) for o in range(octets)]
    for c in range(comps):
        base = jnp.concatenate(
            [jnp.broadcast_to(top[:, c : c + 1], (8, LANES)) for top in tops], axis=0
        )

        def emit(tile, value):
            out_ref[c, :, tile * LANES : (tile + 1) * LANES] = base - value

        inverse_rows(spec, slice(c * points, (c + 1) * points), slabs, emit)


def pack_kernel(dims, displacement_ref, halo_ref, out_ref):
    nodes_part, halo = dims
    moved = displacement_ref[...]
    halo_f = halo_ref[...].astype(F32)
    node_dev = moved.shape[1]
    wide = out_ref.shape[1]
    pieces = [moved[0:1], moved[1:2], moved[2:3]]
    pieces.append(jnp.zeros((1, nodes_part - 3 * node_dev), F32))
    pieces += [halo_f[1:2], halo_f[0:1]]
    pieces.append(jnp.zeros((1, wide - nodes_part - 2 * halo), F32))
    out_ref[...] = jnp.broadcast_to(jnp.concatenate(pieces, axis=1), out_ref.shape)


def on_device(
    displacement, shape_grads, point_weights, conn, halo_nodes, warm_strain, moduli, owner, sweeps
):
    axes = ("mesh", "rve")
    points, comps, voxels = warm_strain.shape
    side = round(voxels ** (1.0 / 3.0))
    tiles = voxels // LANES
    slabs = side // 2
    plane = side * side
    owners = lax.axis_size("rve")
    devices = lax.axis_size("mesh") * owners
    node_dev = displacement.shape[1]
    nodes_part = node_dev * owners
    halo = halo_nodes.shape[1]
    per_owner = max(2, points // owners)
    dense = per_owner * owners == points and owners == 8
    wide = -(-(nodes_part + 2 * halo) // LANES) * LANES
    vmem = pl.BlockSpec(memory_space=pltpu.VMEM)
    hbm = pl.BlockSpec(memory_space=pltpu.HBM)
    smem = pl.BlockSpec(memory_space=pltpu.SMEM)
    params = pltpu.CompilerParams(vmem_limit_bytes=62 << 20)

    packed = pl.pallas_call(
        functools.partial(pack_kernel, (nodes_part, halo)),
        out_shape=jax.ShapeDtypeStruct((devices, wide), F32),
        in_specs=[vmem, vmem],
        out_specs=vmem,
        name="pack",
    )(displacement, halo_nodes)
    table = lax.all_to_all(packed, axes, split_axis=0, concat_axis=0, tiled=True)

    owner_row = owner.reshape(1, points)
    sweeps_row = sweeps.reshape(1, points)
    weight_row = point_weights.reshape(1, points)
    part = lax.axis_index("mesh").astype(jnp.int32).reshape(1)
    place = lax.axis_index("rve").astype(jnp.int32).reshape(1)
    warm = warm_strain.transpose(1, 0, 2)
    moduli_rows = (
        moduli.reshape(points, 2, tiles, LANES).transpose(0, 2, 1, 3).reshape(points, -1, LANES)
    )
    forward, inverse, normals = (jnp.asarray(t) for t in build_tables(side))
    rows = comps * points
    more = (comps + 2) * points
    octets = points // 8
    table_scratch = pltpu.VMEM(forward.shape, BF16)
    spec, both, mean = pl.pallas_call(
        functools.partial(first_kernel, (points, comps, side, owners, dense)),
        out_shape=(
            jax.ShapeDtypeStruct((2, slabs, more, plane), F32),
            jax.ShapeDtypeStruct((tiles, 2 * points, LANES), F32),
            jax.ShapeDtypeStruct((more, LANES), F32),
        ),
        in_specs=[smem, vmem, hbm, hbm, hbm],
        out_specs=(hbm, hbm, vmem),
        scratch_shapes=[
            table_scratch,
            pltpu.VMEM((comps, points, voxels), F32),
            pltpu.VMEM((points * (2 * tiles + 8), LANES), F32),
            pltpu.VMEM((2, slabs, more, plane), F32),
            pltpu.VMEM((tiles, more, LANES), F32),
            pltpu.VMEM((2, slabs, more, plane), BF16),
            pltpu.VMEM((2, slabs, more, plane), BF16),
            pltpu.SemaphoreType.DMA((6,)),
        ],
        compiler_params=params,
        cost_estimate=pl.CostEstimate(
            flops=2 * 3 * 16 * more * plane * plane, transcendentals=0, bytes_accessed=4 << 20
        ),
        name="first",
    )(place, owner_row, warm, moduli_rows, forward)

    dims = (points, comps, side, devices, node_dev, halo, owners, nodes_part, owners, dense)
    block = 3 * 4 * slabs + 3 * (2 * slabs * WINDOW // LANES) + 8
    blocks = owners if dense else 1
    *send, stress, force = pl.pallas_call(
        functools.partial(second_kernel, dims),
        out_shape=(
            *(jax.ShapeDtypeStruct((points * block // blocks, LANES), F32),) * blocks,
            jax.ShapeDtypeStruct((8, LANES), F32),
            jax.ShapeDtypeStruct((devices, LANES), F32),
        ),
        in_specs=[smem] * 2 + [vmem] * 8 + [hbm] * 4,
        out_specs=(vmem,) * (blocks + 2),
        scratch_shapes=[
            pltpu.VMEM((points * block, LANES), F32),
            pltpu.VMEM((2, slabs, more, plane), F32),
            pltpu.VMEM((tiles, 2 * points, LANES), F32),
            table_scratch,
            table_scratch,
            pltpu.VMEM((tiles, rows, LANES), F32),
            pltpu.VMEM((2, slabs, rows, plane), BF16),
            pltpu.VMEM((2, slabs, rows, plane), BF16),
            pltpu.VMEM((2, slabs, rows, plane), F32),
            pltpu.VMEM((octets, 3 * 4 * slabs, 8, LANES), F32),
            pltpu.VMEM((octets, 3, 2 * slabs, 8, LANES), F32),
            pltpu.VMEM((octets, 3, 2, 8, LANES), F32),
            pltpu.VMEM((comps, points, LANES), F32),
            pltpu.SemaphoreType.DMA((3,)),
            pltpu.SemaphoreType.DMA((slabs,)),
        ],
        compiler_params=params,
        cost_estimate=pl.CostEstimate(
            flops=2 * 2 * 3 * 16 * rows * plane * plane, transcendentals=0, bytes_accessed=6 << 20
        ),
        name="second",
    )(
        part, place, owner_row, sweeps_row, weight_row, conn.T, shape_grads, table, mean, normals,
        spec, both, forward, inverse,
    )

    finish = pl.pallas_call(
        functools.partial(third_kernel, (points, comps, side, blocks)),
        out_shape=jax.ShapeDtypeStruct((comps, points, voxels), F32),
        in_specs=[smem] + [vmem] * (blocks + 1) + [hbm],
        out_specs=vmem,
        scratch_shapes=[
            pltpu.VMEM((points * block, LANES), F32),
            table_scratch,
            pltpu.VMEM((2, slabs, rows, plane), BF16),
            pltpu.VMEM((2, slabs, rows, plane), BF16),
            pltpu.VMEM((2, slabs, rows, plane), F32),
            pltpu.SemaphoreType.DMA,
        ],
        compiler_params=pltpu.CompilerParams(vmem_limit_bytes=24 << 20),
        cost_estimate=pl.CostEstimate(
            flops=2 * 3 * 16 * rows * plane * plane, transcendentals=0, bytes_accessed=4 << 20
        ),
        name="third",
    )
    comps_out = stress[:comps, :points]
    if dense:
        arrived = [send[0]] + [
            lax.ppermute(send[i], "rve", [(j, (j + i) % owners) for j in range(owners)])
            for i in range(1, owners)
        ]
        micro = finish(place, *arrived, normals, inverse).transpose(1, 0, 2)
    else:
        slots = owners * per_owner
        final = finish(place, send[0], normals, inverse).transpose(1, 0, 2)
        order = jnp.arange(points, dtype=jnp.int32)
        same = owner[:, None] == owner[None, :]
        rank = jnp.sum((same & (order[None, :] < order[:, None])).astype(jnp.int32), axis=1)
        slot = owner * per_owner + rank
        fields = jnp.zeros((slots, comps, voxels), F32).at[slot].set(final)
        flags = jnp.zeros((slots,), F32).at[slot].set(1.0)
        fields = lax.all_to_all(fields, "rve", split_axis=0, concat_axis=0, tiled=True)
        flags = lax.all_to_all(flags, "rve", split_axis=0, concat_axis=0, tiled=True)
        filled = jnp.nonzero(flags > 0.5, size=points)[0].astype(jnp.int32)
        micro = fields[filled]
    pieces = lax.all_to_all(force, axes, split_axis=0, concat_axis=0, tiled=True)
    nodal = jnp.sum(pieces, axis=0)[: 3 * node_dev].reshape(3, node_dev)
    return (nodal, comps_out, micro)


def solution(mesh):
    both = ("mesh", "rve")
    in_specs = (
        P(None, both), P(None, None, both), P(both), P(None, both), P(None, "mesh"),
        P(both, None, None), P(both, None, None), P(both), P(both),
    )
    out_specs = (P(None, both), P(None, both), P(both, None, None))

    return jax.shard_map(
        on_device, mesh=mesh, in_specs=in_specs, out_specs=out_specs, check_vma=False
    )
```
